32 devices in a mesh: group: 4 (over y, core), rep: 8 (over z, x).
Axes of the slice: x: 2, y: 2, z: 4, core: 2. Of those that a mesh axis runs over, the one named last changes fastest.
Arguments:
- table_hot: bfloat16 [32768, 512], P(('group', 'rep')), may hold values from -6 to 6
- table_mid: bfloat16 [131072, 128], P(('group', 'rep')), may hold values from -6 to 6
- table_cold: bfloat16 [131072, 128], P(('group', 'rep')), may hold values from -6 to 6
- proj_hot: bfloat16 [512, 256], replicated, may hold values from -0.25 to 0.25
- proj_mid: bfloat16 [128, 256], replicated, may hold values from -0.5 to 0.5
- proj_cold: bfloat16 [32, 256], replicated, may hold values from -1 to 1
- tower_in: bfloat16 [256, 1024], replicated, may hold values from -0.375 to 0.375
- tower_out: bfloat16 [1024, 256], replicated, may hold values from -0.1875 to 0.1875
- queries: bfloat16 [16384, 256], P(('group', 'rep')), may hold values from -68 to 68
- labels: int32 [16384], P(('group', 'rep')), may hold values from 0 to 4095
- item_slot: int32 [32, 4, 1024], P(('group', 'rep')), may hold values from 0 to 255
- item_block: int32 [32, 4, 1024], P(('group', 'rep')), may hold values from 0 to 2
- serve_rows: int32 [32, 3, 256], P(('group', 'rep')), may hold values from 0 to 16383, as said below
Outputs:
- query_loss: float32 [16384], P(('group', 'rep'))
- query_grad: float32 [16384, 256], P(('group', 'rep'))
- grad_hot: float32 [32768, 512], P(('group', 'rep'))
- grad_mid: float32 [131072, 128], P(('group', 'rep'))
- grad_cold: float32 [131072, 128], P(('group', 'rep'))
- grad_proj_hot: float32 [512, 256], P(None, 'rep')
- grad_proj_mid: float32 [128, 256], P(None, 'rep')
- grad_proj_cold: float32 [32, 256], P(None, 'rep')
- grad_tower_in: float32 [256, 1024], P(None, 'rep')
- grad_tower_out: float32 [1024, 256], P(None, 'rep')
The draws below stay inside these ranges and needn't reach their ends.
Inputs may be any that keep to these rules, and one draw needn't show every extreme that they name: serve_rows[o, b, d * 8 + c] is a row of owner o's shard of block b that requester d sees in slot c; for block 0 it is below 1024, for block 1 below 4096, for block 2 below 16384; the 8 rows that one owner serves to one requester in one block are distinct.
All inputs are finite; a program needn't handle non-finite values.
Results may differ from the reference program's by a relative error of at most 0.02.
The reference program's roundings to bfloat16 on the way count: a program that leaves them out, or rounds other values in their place, can miss the bound.
Values may be sent and summed in bfloat16 or wider, within the bound.
No kernel may reach another device: no remote copies, remote signals or barrier semaphores. Data moves between devices by JAX's collectives and lax.ppermute only.
A program may use at most 128 MiB of HBM per device.

```python
import math
import jax
import jax.numpy as jnp
import numpy as np
from jax import lax

D = 256
H = 1024
W_HOT = 512
W_MID = 128
W_COLD = 32
FIELDS = 4
CAP = 8
ITEMS_DEV = 1024
Q_DEV = 512
R_HOT_DEV = 1024
R_MID_DEV = 4096
R_COLD_DEV = 16384
SLOTS = 256
N_GROUP = 4
N_REP = 8


def draw_queries(key, part):
    full_shape = (N_GROUP * N_REP * Q_DEV, D)
    first_key = jax.random.fold_in(jax.random.fold_in(key, 11), 0)
    return jnp.clip(jax.random.normal(first_key, full_shape, jnp.float32), -4.0, 4.0).astype(jnp.bfloat16)


def draw_serve_rows(key, part):
    devices = N_GROUP * N_REP
    slot_total = devices * CAP
    stride = jnp.array([R_HOT_DEV // CAP, R_MID_DEV // CAP, R_COLD_DEV // CAP], jnp.int32)
    offset = jax.random.randint(jax.random.fold_in(key, 23), (devices, 3, slot_total), 0, 1 << 20) % stride[None, :, None]
    slot_pos = jnp.arange(slot_total, dtype=jnp.int32) % CAP
    return (slot_pos[None, None, :] * stride[None, :, None] + offset).astype(jnp.int32)


def with_ends(values, key, least, largest):
    shape = values.shape
    index_at = [jax.random.randint(jax.random.fold_in(key, axis), (), 0, shape[axis]) for axis in range(len(shape))]
    values = values.at[tuple(index_at)].set(least)
    longest = shape.index(max(shape))
    index_at[longest] = (index_at[longest] + 1) % shape[longest]
    return values.at[tuple(index_at)].set(largest)


def shard_levels(key, dims, cuts, smallest, top_value):
    def one(axis_at, parts):
        draws = jax.random.uniform(jax.random.fold_in(jax.random.fold_in(key, 6), axis_at), (parts,), jnp.float32, smallest / len(cuts), top_value / len(cuts))
        return jnp.repeat(jnp.exp(draws), dims[axis_at] // parts).reshape((-1,) + (1,) * (len(dims) - axis_at - 1))

    factor_of = one(*cuts[0])
    for cut in cuts[1:]:
        factor_of = factor_of * one(*cut)
    return factor_of


def rank_table(count, skew):
    loads = [(1 << 20) // math.isqrt(standing ** skew) + 1 for standing in range(1, count + 1)]
    scale = 1 + sum(loads) // (1 << 30)
    return np.cumsum(np.array([max(1, weight // scale) for weight in loads]))


def ranked(stream_key, extent, number_of, skew):
    table = rank_table(number_of, skew)
    ticket = jax.random.randint(jax.random.fold_in(stream_key, 1), extent, 0, int(table[number_of - 1]))
    standing = jnp.searchsorted(jnp.asarray(table, jnp.int32), ticket, side="right")
    return jax.random.permutation(jax.random.fold_in(stream_key, 2), number_of)[standing].astype(jnp.int32)


def scatter_about(rng, dims, scale, reach, cuts=(), kind=jnp.bfloat16):
    drawn = jax.random.normal(rng, dims, jnp.float32) * scale
    if len(cuts) > 0:
        drawn = shard_levels(rng, dims, cuts, -0.22, 0.18) * drawn
    return jnp.clip(drawn, min=-reach, max=reach).astype(kind)


def setup_inputs(seed: int = 0) -> dict:
    seeds = jax.random.split(jax.random.key(seed), 14)
    table_hot = scatter_about(seeds[0], (N_GROUP * N_REP * R_HOT_DEV, W_HOT), 1.0, 6.0, ((0, 32),))
    table_mid = scatter_about(seeds[1], (N_GROUP * N_REP * R_MID_DEV, W_MID), 1.0, 6.0, ((0, 32),))
    table_cold = scatter_about(seeds[2], (N_GROUP * N_REP * R_COLD_DEV // 4, 4 * W_COLD), 1.0, 6.0, ((0, 32),))
    proj_hot = scatter_about(seeds[3], (W_HOT, D), W_HOT ** -0.5, 0.25)
    proj_mid = scatter_about(seeds[4], (W_MID, D), W_MID ** -0.5, 0.5)
    proj_cold = scatter_about(seeds[5], (W_COLD, D), W_COLD ** -0.5, 1.0)
    tower_in = scatter_about(seeds[6], (D, H), D ** -0.5, 0.375)
    tower_out = scatter_about(seeds[7], (H, D), H ** -0.5, 0.1875)
    queries = draw_queries(jax.random.fold_in(seeds[13], 71), 0)
    labels = with_ends(jax.random.randint(seeds[9], (N_GROUP * N_REP * Q_DEV,), 0, N_GROUP * ITEMS_DEV), jax.random.fold_in(seeds[9], 1), 0, (N_GROUP * ITEMS_DEV) - 1).astype(jnp.int32)
    item_slot = with_ends(ranked(seeds[10], (N_GROUP * N_REP, FIELDS, ITEMS_DEV), SLOTS, 1), jax.random.fold_in(seeds[10], 3), 0, SLOTS - 1).astype(jnp.int32)
    item_block = with_ends(jax.random.randint(seeds[11], (N_GROUP * N_REP, FIELDS, ITEMS_DEV), 0, 3), jax.random.fold_in(seeds[11], 1), 0, 2).astype(jnp.int32)
    serve_rows = draw_serve_rows(jax.random.fold_in(seeds[13], 71), 0)
    return {"table_hot": table_hot, "table_mid": table_mid, "table_cold": table_cold, "proj_hot": proj_hot, "proj_mid": proj_mid, "proj_cold": proj_cold, "tower_in": tower_in, "tower_out": tower_out, "queries": queries, "labels": labels, "item_slot": item_slot, "item_block": item_block, "serve_rows": serve_rows}


NORM_EPS = 1e-06
LOGIT_SCALE = 0.2

def silu_slope(pre_act):
    sigmoid = jax.nn.sigmoid(pre_act)
    return sigmoid * (1.0 + pre_act * (1.0 - sigmoid))

def pick_cold(cold_lines, row_ids, col_width):
    pieces = cold_lines.reshape(cold_lines.shape[0], 4, col_width)
    select = jnp.arange(4, dtype=jnp.int32)[None, :] == (row_ids % 4).astype(jnp.int32)[:, None]
    return lax.optimization_barrier(jnp.sum(jnp.where(select[:, :, None], pieces, jnp.zeros((), pieces.dtype)), axis=1)).astype(pieces.dtype)

def cold_add(row_ids, values):
    select = (jnp.arange(4, dtype=jnp.int32)[None, :] == (row_ids % 4).astype(jnp.int32)[:, None]).astype(jnp.float32)
    spread = (select[:, :, None] * values[:, None, :]).reshape(row_ids.shape[0], 4 * W_COLD)
    return jnp.zeros((R_COLD_DEV // 4, 4 * W_COLD), jnp.float32).at[(row_ids // 4).astype(jnp.int32)].add(spread)

def contract(left_rows, right_rows):
    return lax.dot_general(left_rows, right_rows, (((0,), (0,)), ((), ())), preferred_element_type=jnp.float32)

def unproject(slot_grad, weight):
    return lax.dot_general(slot_grad, weight, (((1,), (1,)), ((), ())), preferred_element_type=jnp.float32)

def reference(table_hot, table_mid, table_cold, proj_hot, proj_mid, proj_cold, tower_in, tower_out, queries, labels, item_slot, item_block, serve_rows):
    devices = N_GROUP * N_REP
    slot_total = devices * CAP
    hot_shards = table_hot.reshape(devices, R_HOT_DEV, W_HOT)
    mid_shards = table_mid.reshape(devices, R_MID_DEV, W_MID)
    cold_shards = table_cold.reshape(devices, R_COLD_DEV // 4, 4 * W_COLD)
    owner_hot = jax.vmap(lambda shard_table, row_ids: shard_table[row_ids])(hot_shards, serve_rows[:, 0])
    owner_mid = jax.vmap(lambda shard_table, row_ids: shard_table[row_ids])(mid_shards, serve_rows[:, 1])
    owner_cold = jax.vmap(lambda shard_table, row_ids: pick_cold(shard_table[row_ids // 4], row_ids, W_COLD))(cold_shards, serve_rows[:, 2])

    def to_requester(owned):
        col_width = owned.shape[-1]
        return owned.reshape(devices, devices, CAP, col_width).transpose(1, 0, 2, 3).reshape(devices * slot_total, col_width)
    raw_hot = to_requester(owner_hot)
    raw_mid = to_requester(owner_mid)
    raw_cold = to_requester(owner_cold)

    def project(raw_rows, weight):
        return jnp.dot(raw_rows, weight, preferred_element_type=jnp.float32).astype(jnp.bfloat16).reshape(devices, slot_total, D)
    slot_table = jnp.concatenate([project(raw_hot, proj_hot), project(raw_mid, proj_mid), project(raw_cold, proj_cold)], axis=1)
    slot_index = (item_block * slot_total + item_slot).astype(jnp.int32)
    gathered = jax.vmap(lambda table_rows, which: table_rows[which])(slot_table, slot_index)
    pooled = lax.optimization_barrier(jnp.sum(gathered.astype(jnp.float32), axis=1)).astype(jnp.bfloat16).reshape(devices * ITEMS_DEV, D)
    pre_act = jnp.dot(pooled, tower_in, preferred_element_type=jnp.float32)
    hidden = jax.nn.silu(pre_act).astype(jnp.bfloat16)
    residual = pooled.astype(jnp.float32) + jnp.dot(hidden, tower_out, preferred_element_type=jnp.float32)
    inv_rms = lax.rsqrt(lax.optimization_barrier(jnp.mean(residual * residual, axis=1, keepdims=True)) + NORM_EPS)
    vectors = (residual * inv_rms).astype(jnp.bfloat16)
    negatives = vectors.reshape(N_GROUP, N_REP, ITEMS_DEV, D).transpose(1, 0, 2, 3).reshape(N_REP, N_GROUP * ITEMS_DEV, D)
    group_queries = queries.reshape(N_GROUP, N_REP, Q_DEV, D).transpose(1, 0, 2, 3).reshape(N_REP, N_GROUP * Q_DEV, D)
    group_labels = labels.reshape(N_GROUP, N_REP, Q_DEV).transpose(1, 0, 2).reshape(N_REP, N_GROUP * Q_DEV)

    def one_group(group_args):
        negs_here, queries_here, labels_here = group_args
        scores = lax.dot_general(queries_here, negs_here, (((1,), (1,)), ((), ())), preferred_element_type=jnp.float32) * LOGIT_SCALE
        row_max = lax.optimization_barrier(jnp.max(scores, axis=1, keepdims=True))
        log_total = row_max[:, 0] + jnp.log(lax.optimization_barrier(jnp.sum(jnp.exp(scores - row_max), axis=1)))
        onehot = jnp.arange(scores.shape[1], dtype=jnp.int32)[None, :] == labels_here[:, None]
        picked = lax.optimization_barrier(jnp.sum(jnp.where(onehot, scores, jnp.zeros((), jnp.float32)), axis=1))
        score_grad = (jnp.exp(scores - log_total[:, None]) - onehot.astype(jnp.float32)).astype(jnp.bfloat16)
        query_grad = LOGIT_SCALE * jnp.dot(score_grad, negs_here, preferred_element_type=jnp.float32)
        neg_grad = LOGIT_SCALE * contract(score_grad, queries_here)
        return (log_total - picked, query_grad, neg_grad)
    loss_all, qgrad_all, neg_grad = lax.map(one_group, (negatives, group_queries, group_labels))
    query_loss = loss_all.reshape(N_REP, N_GROUP, Q_DEV).transpose(1, 0, 2).reshape(-1)
    query_grad = qgrad_all.reshape(N_REP, N_GROUP, Q_DEV, D).transpose(1, 0, 2, 3).reshape(-1, D)
    vec_grad = neg_grad.reshape(N_REP, N_GROUP, ITEMS_DEV, D).transpose(1, 0, 2, 3).reshape(-1, D)
    dot_wide = lax.optimization_barrier(jnp.sum(vec_grad * residual, axis=1, keepdims=True))
    wide_grad = inv_rms * vec_grad - inv_rms ** 3 / D * residual * dot_wide
    wide_low = wide_grad.astype(jnp.bfloat16)
    hidden_grad = unproject(wide_low, tower_out)
    pre_grad = (hidden_grad * silu_slope(pre_act)).astype(jnp.bfloat16)
    pooled_grad = (unproject(pre_grad, tower_in) + wide_grad).astype(jnp.bfloat16).reshape(devices, ITEMS_DEV, D)

    def slot_sum(item_grad, which):
        stacked = jnp.broadcast_to(item_grad.astype(jnp.float32)[None], (FIELDS, ITEMS_DEV, D)).reshape(-1, D)
        return jax.ops.segment_sum(stacked, which.reshape(-1), num_segments=3 * slot_total)
    slot_grad = jax.vmap(slot_sum)(pooled_grad, slot_index).astype(jnp.bfloat16)
    grad_hot_slots = slot_grad[:, :slot_total].reshape(-1, D)
    grad_mid_slots = slot_grad[:, slot_total:2 * slot_total].reshape(-1, D)
    grad_cold_slots = slot_grad[:, 2 * slot_total:].reshape(-1, D)

    def to_owner(values):
        col_width = values.shape[-1]
        return values.reshape(devices, devices, CAP, col_width).transpose(1, 0, 2, 3).reshape(devices, slot_total, col_width)
    back_hot = to_owner(unproject(grad_hot_slots, proj_hot))
    back_mid = to_owner(unproject(grad_mid_slots, proj_mid))
    back_cold = to_owner(unproject(grad_cold_slots, proj_cold))
    grad_hot = jax.vmap(lambda row_ids, values: jnp.zeros((R_HOT_DEV, W_HOT), jnp.float32).at[row_ids].add(values))(serve_rows[:, 0], back_hot).reshape(-1, W_HOT)
    grad_mid = jax.vmap(lambda row_ids, values: jnp.zeros((R_MID_DEV, W_MID), jnp.float32).at[row_ids].add(values))(serve_rows[:, 1], back_mid).reshape(-1, W_MID)
    grad_cold = jax.vmap(cold_add)(serve_rows[:, 2], back_cold).reshape(-1, 4 * W_COLD)
    grad_proj_hot = contract(raw_hot, grad_hot_slots)
    grad_proj_mid = contract(raw_mid, grad_mid_slots)
    grad_proj_cold = contract(raw_cold, grad_cold_slots)
    grad_tower_in = contract(pooled, pre_grad)
    grad_tower_out = contract(hidden, wide_low)
    return (query_loss, query_grad, grad_hot, grad_mid, grad_cold, grad_proj_hot, grad_proj_mid, grad_proj_cold, grad_tower_in, grad_tower_out)
```

```python
import functools

import jax
import jax.numpy as jnp
from jax import lax
from jax.experimental import pallas as pl
from jax.experimental.pallas import tpu as pltpu
from jax.sharding import PartitionSpec as P

NORM_EPS = 1e-06
LOGIT_SCALE = 0.2
AXES = ("group", "rep")
LANES = 128
QB = 256
IB = 256
MIB = 1 << 20
F32 = jnp.float32
BF16 = jnp.bfloat16

NN = (((1,), (0,)), ((), ()))
NT = (((1,), (1,)), ((), ()))
TN = (((0,), (0,)), ((), ()))


def mm(left, right, dims=NN):
    return lax.dot_general(left, right, dims, preferred_element_type=F32)


def ones_where(mask):
    return jnp.where(mask, jnp.float32(1), jnp.float32(0))


def iota(shape, dim):
    return lax.broadcasted_iota(jnp.int32, shape, dim)


def call(body, out_shape, inputs, scratch=(), vmem=40, name=None):
    spec = pl.BlockSpec(memory_space=pltpu.VMEM)
    return pl.pallas_call(
        body,
        out_shape=out_shape,
        in_specs=[spec] * len(inputs),
        out_specs=jax.tree.map(lambda _: spec, out_shape),
        scratch_shapes=list(scratch),
        compiler_params=pltpu.CompilerParams(vmem_limit_bytes=vmem * MIB),
        name=name,
    )(*inputs)


def sds(shape, dtype):
    return jax.ShapeDtypeStruct(shape, dtype)


def columns_of(rows_ref, pad_ref):
    pad_ref[...] = jnp.zeros_like(pad_ref)
    pad_ref[0 : rows_ref.shape[1], :] = rows_ref[0]
    return pad_ref[...].T


def gather_body(steps, cold_width, served, hot, mid, cold, out, pad, idx, acc):
    step = pl.program_id(0)
    slots = idx.shape[0]
    w_hot, w_mid = hot.shape[1], mid.shape[1]

    @pl.when(step == 0)
    def _():
        idx[...] = columns_of(served, pad)
        acc[...] = jnp.zeros_like(acc)

    def pick(table, col, at):
        block = table.shape[0]
        hit = iota((slots, block), 1) + step * block == col
        acc[:, at : at + table.shape[1]] += mm(ones_where(hit).astype(BF16), table[...])

    pick(hot, idx[:, 0:1], 0)
    pick(mid, idx[:, 1:2], w_hot)
    pick(cold, lax.shift_right_logical(idx[:, 2:3], 2), w_hot + w_mid)

    @pl.when(step == steps - 1)
    def _():
        out[:, 0 : w_hot + w_mid] = acc[:, 0 : w_hot + w_mid].astype(BF16)
        lines = acc[:, w_hot + w_mid :]
        mine = lax.div(iota(lines.shape, 1), cold_width) == (idx[:, 2:3] & 3)
        out[:, w_hot + w_mid :] = jnp.where(mine, lines, 0.0).astype(BF16)


def gather_rows(serve_rows, table_hot, table_mid, table_cold, cold_width):
    slots = serve_rows.shape[2]
    width = table_hot.shape[1] + table_mid.shape[1] + table_cold.shape[1]
    steps = 8

    def blocked(table):
        return pl.BlockSpec((table.shape[0] // steps, table.shape[1]), lambda i: (i, 0))

    return pl.pallas_call(
        functools.partial(gather_body, steps, cold_width),
        grid=(steps,),
        out_shape=sds((slots, width), BF16),
        in_specs=[
            pl.BlockSpec(serve_rows.shape, lambda i: (0, 0, 0)),
            blocked(table_hot),
            blocked(table_mid),
            blocked(table_cold),
        ],
        out_specs=pl.BlockSpec((slots, width), lambda i: (0, 0)),
        scratch_shapes=[
            pltpu.VMEM((8, slots), jnp.int32),
            pltpu.VMEM((slots, 8), jnp.int32),
            pltpu.VMEM((slots, width), F32),
        ],
        compiler_params=pltpu.CompilerParams(vmem_limit_bytes=24 * MIB),
        name="gather_rows",
    )(serve_rows, table_hot, table_mid, table_cold)


def count_body(slots, item_slot, item_block, by_item, by_slot, pad):
    fields, items = item_slot.shape[1], item_slot.shape[2]
    which = item_block[0] * slots + item_slot[0]
    pad[...] = jnp.zeros_like(pad)
    pad[0:fields, :] = which
    cols = pad[...].T
    for base in range(0, by_slot.shape[0], QB):
        rows = iota((QB, items), 0) + base
        total = jnp.zeros((QB, items), F32)
        for f in range(fields):
            total += ones_where(rows == which[f : f + 1, :])
        by_slot[base : base + QB, :] = total.astype(BF16)
        lanes = iota((items, QB), 1) + base
        total = jnp.zeros((items, QB), F32)
        for f in range(fields):
            total += ones_where(lanes == cols[:, f : f + 1])
        by_item[:, base : base + QB] = total.astype(BF16)


def tall(weight, times):
    return jnp.concatenate([weight] * times, axis=0)


def label_rows(label, base, jj):
    return label[0:1, jj * QB : (jj + 1) * QB] - base


def forward_body(peers, raw, counts, p_hot, p_mid, p_cold, t_in, t_out, *rest):
    queries, labels = rest[:peers], rest[peers : 2 * peers]
    pooled_o, resid_o, vec_o, stats_o, table = rest[2 * peers :]
    slots = raw.shape[0]
    w_hot, w_mid = p_hot.shape[0], p_mid.shape[0]
    w_cold = raw.shape[1] - w_hot - w_mid
    table[0:slots, :] = mm(raw[:, 0:w_hot], p_hot[...]).astype(BF16)
    table[slots : 2 * slots, :] = mm(raw[:, w_hot : w_hot + w_mid], p_mid[...]).astype(BF16)
    table[2 * slots :, :] = mm(
        raw[:, w_hot + w_mid :], tall(p_cold[...], w_cold // p_cold.shape[0])
    ).astype(BF16)
    items = counts.shape[0]
    for at in range(0, items, IB):
        rows = slice(at, at + IB)
        pooled = mm(counts[rows, :], table[...]).astype(BF16)
        pre = mm(pooled, t_in[...])
        hidden = (pre * jax.nn.sigmoid(pre)).astype(BF16)
        resid = pooled.astype(F32) + mm(hidden, t_out[...])
        inv = lax.rsqrt(jnp.mean(resid * resid, axis=1, keepdims=True) + NORM_EPS)
        pooled_o[rows, :] = pooled
        resid_o[rows, :] = resid
        vec_o[rows, :] = (resid * inv).astype(BF16)
    base = lax.axis_index("group") * items
    per = queries[0].shape[0] // QB
    for t in range(peers):
        for jj in range(per):
            s = mm(vec_o[...], queries[t][jj * QB : (jj + 1) * QB, :], NT) * LOGIT_SCALE
            top = jnp.max(s, axis=0, keepdims=True)
            total = jnp.sum(jnp.exp(s - top), axis=0, keepdims=True)
            hit = iota(s.shape, 0) == label_rows(labels[t], base, jj)
            picked = jnp.sum(jnp.where(hit, s, 0.0), axis=0, keepdims=True)
            j = t * per + jj
            stats_o[j : j + 1, 0:QB] = top
            stats_o[j : j + 1, QB : 2 * QB] = total
            stats_o[j : j + 1, 2 * QB :] = picked


class Plan:
    def __init__(self, groups, reps, width, inner, raw_width):
        self.groups, self.reps = groups, reps
        self.ky = groups // 2
        self.kx, self.kz = 2, reps // 2
        self.hr = inner // reps
        self.dr = width // reps
        self.b_in = width // LANES
        self.b_out = inner // LANES
        self.b_raw = raw_width // LANES
        rows = self.hr * self.b_in + self.dr * (self.b_out + self.b_raw)
        unit = 16 * self.ky
        units = -(-rows // (2 * unit))
        self.half = units * unit
        self.m1 = -(-units // 2) * 16
        self.m2 = units * 16 - self.m1
        self.rows = 2 * self.half
        self.used = rows
        self.p1 = reps * self.ky * self.m1
        self.p2 = reps * self.ky * self.m2


def backward_body(plan, peers, loss_dtype, *refs):
    stats, refs = refs[:peers], refs[peers:]
    queries, refs = refs[:peers], refs[peers:]
    labels, refs = refs[:peers], refs[peers:]
    vec, resid, pooled, by_slot, raw, p_hot, p_mid, p_cold, t_in, t_out = refs[:10]
    loss_o, grad_o, keep_o, send_o, back_o = refs[10:15]
    wide_s, low_s, hid_s, pre_s, pgrad_s, slot_s, chunk = refs[15:]
    items, width = vec.shape
    nq = queries[0].shape[0]
    per = nq // QB
    me_g, me_r = lax.axis_index("group"), lax.axis_index("rep")
    base = me_g * items
    for t in range(peers):
        for jj in range(per):
            rows = [(t ^ s) * per + jj for s in range(peers)]
            tops = [stats[s][rows[s] : rows[s] + 1, 0:QB] for s in range(peers)]
            totals = [stats[s][rows[s] : rows[s] + 1, QB : 2 * QB] for s in range(peers)]
            top = functools.reduce(jnp.maximum, tops)
            total = sum(tot * jnp.exp(m - top) for m, tot in zip(tops, totals))
            log_total = top + jnp.log(total)
            if t == 0:
                picked = sum(stats[s][rows[s] : rows[s] + 1, 2 * QB :] for s in range(peers))
                loss_o[0:1, jj * QB : (jj + 1) * QB] = log_total - picked
            s = mm(vec[...], queries[t][jj * QB : (jj + 1) * QB, :], NT) * LOGIT_SCALE
            hit = iota(s.shape, 0) == label_rows(labels[t], base, jj)
            grad = jnp.exp(s - log_total) - ones_where(hit)
            at = t * nq + jj * QB
            grad_o[:, at : at + QB] = grad.astype(BF16)
    for at in range(0, items, IB):
        rows = slice(at, at + IB)
        vgrad = mm(grad_o[rows, 0:nq], queries[0][...])
        for t in range(1, peers):
            vgrad += mm(grad_o[rows, t * nq : (t + 1) * nq], queries[t][...])
        vgrad = LOGIT_SCALE * vgrad
        res = resid[rows, :]
        inv = lax.rsqrt(jnp.mean(res * res, axis=1, keepdims=True) + NORM_EPS)
        dot_wide = jnp.sum(vgrad * res, axis=1, keepdims=True)
        wide = inv * vgrad - (inv * inv * inv / width * dot_wide) * res
        low = wide.astype(BF16)
        low_s[rows, :] = low
        pre = mm(pooled[rows, :], t_in[...])
        sig = jax.nn.sigmoid(pre)
        hid_s[rows, :] = (pre * sig).astype(BF16)
        pre_g = (mm(low, t_out[...], NT) * (sig * (1.0 + pre * (1.0 - sig)))).astype(BF16)
        pre_s[rows, :] = pre_g
        pgrad_s[rows, :] = (mm(pre_g, t_in[...], NT) + wide).astype(BF16)
    slots = raw.shape[0]
    w_hot, w_mid = p_hot.shape[0], p_mid.shape[0]
    w_cold = raw.shape[1] - w_hot - w_mid
    slot_s[...] = mm(by_slot[...], pgrad_s[...]).astype(BF16)
    back_o[:, 0:width] = slot_s[0:slots, :]
    back_o[:, width : width + w_mid] = mm(slot_s[slots : 2 * slots, :], p_mid[...], NT).astype(BF16)
    back_o[:, width + w_mid :] = mm(
        slot_s[2 * slots :, :], tall(p_cold[...], w_cold // p_cold.shape[0]), NT
    ).astype(BF16)

    g_in = mm(pooled[...], pre_s[...], TN).T
    hr, dr = plan.hr, plan.dr
    for r in range(plan.reps):
        for b in range(plan.b_in):
            chunk[r, b * hr : (b + 1) * hr, :] = g_in[
                r * hr : (r + 1) * hr, b * LANES : (b + 1) * LANES
            ].astype(BF16)
    at = hr * plan.b_in
    g_out = mm(low_s[...], hid_s[...], TN)
    parts = [(g_out, plan.b_out)]
    lane = 0
    for b, w in enumerate((w_hot, w_mid, w_cold)):
        parts.append(
            (mm(slot_s[b * slots : (b + 1) * slots, :], raw[:, lane : lane + w], TN), w // LANES)
        )
        lane += w
    for value, blocks in parts:
        for r in range(plan.reps):
            for b in range(blocks):
                chunk[r, at + b * dr : at + (b + 1) * dr, :] = value[
                    r * dr : (r + 1) * dr, b * LANES : (b + 1) * LANES
                ].astype(BF16)
        at += blocks * dr
    if plan.rows > plan.used:
        chunk[:, plan.used :, :] = jnp.zeros((plan.reps, plan.rows - plan.used, LANES), BF16)
    core, me_y = me_g & 1, lax.shift_right_logical(me_g, 1)
    for h, out in ((0, keep_o), (1, send_o)):
        start = (core ^ h) * plan.half
        for z in range(plan.kz):
            for x in range(plan.kx):
                r = me_r ^ (z * 2 + x)
                for y in range(plan.ky):
                    q = me_y ^ y
                    m = plan.m1
                    at = ((x * plan.ky + y) * plan.kz + z) * m
                    row = pl.multiple_of(start + q * m, 16)
                    out[at : at + m, :] = chunk[r, pl.ds(row, m), :]
                    m = plan.m2
                    if m:
                        at = plan.p1 + ((y * plan.kx + x) * plan.kz + z) * m
                        row = pl.multiple_of(start + plan.ky * plan.m1 + q * m, 16)
                        out[at : at + m, :] = chunk[r, pl.ds(row, m), :]


def query_grad_body(peers, vec, grad, keep_o, send_o):
    turned = vec[...].T
    nq = keep_o.shape[2]
    for t in range(peers):
        part = (LOGIT_SCALE * mm(turned, grad[:, t * nq : (t + 1) * nq])).astype(BF16)
        (send_o if t & 1 else keep_o)[t // 2] = part


def query_core_body(keep, got, own_o, *sends):
    own_o[...] = keep[0].astype(F32) + got[0].astype(F32)
    for y, out in enumerate(sends):
        out[...] = (keep[y + 1].astype(F32) + got[y + 1].astype(F32)).astype(BF16)


def query_final_body(own, *rest):
    got, out = rest[:-1], rest[-1]
    total = own[...]
    for part in got:
        total += part[...].astype(F32)
    out[...] = total.T


def cut_body(sources, cuts, *refs):
    n_in = len(refs) - len(cuts)
    for out, pieces in zip(refs[n_in:], cuts):
        for at, rows, terms in pieces:
            total = None
            for i, first in terms:
                part = refs[i][first : first + rows, :].astype(F32)
                total = part if total is None else total + part
            out[at : at + rows, :] = total.astype(out.dtype)


def cut(inputs, cuts, name):
    shapes = [sds((sum(p[1] for p in pieces), LANES), BF16) for pieces in cuts]
    return call(
        functools.partial(cut_body, None, cuts), shapes, inputs, vmem=16, name=name
    )


def final_body(plan, w_hot, w_mid, w_cold, cold_rows, *refs):
    pieces = refs[: plan.groups]
    o_in, o_out, o_hot, o_mid, o_cold, chunk = refs[plan.groups :]
    me_g = lax.axis_index("group")
    for t in range(plan.groups):
        h = (me_g & 1) ^ (t & 1)
        q = lax.shift_right_logical(me_g, 1) ^ (t >> 1)
        start = h * plan.half
        row = pl.multiple_of(start + q * plan.m1, 16)
        chunk[pl.ds(row, plan.m1), :] = pieces[t][0 : plan.m1, :].astype(F32)
        if plan.m2:
            row = pl.multiple_of(start + plan.ky * plan.m1 + q * plan.m2, 16)
            chunk[pl.ds(row, plan.m2), :] = pieces[t][plan.m1 :, :].astype(F32)
    hr, dr = plan.hr, plan.dr
    for b in range(plan.b_in):
        o_in[b * LANES : (b + 1) * LANES, :] = chunk[b * hr : (b + 1) * hr, :].T
    at = hr * plan.b_in
    for out, w in ((o_out, plan.b_out * LANES), (o_hot, w_hot), (o_mid, w_mid)):
        for b in range(w // LANES):
            out[b * LANES : (b + 1) * LANES, :] = chunk[at : at + dr, :].T
            at += dr
    total = jnp.zeros((cold_rows, dr), F32)
    for b in range(w_cold // LANES):
        turned = chunk[at : at + dr, :].T
        for k in range(LANES // cold_rows):
            total += turned[k * cold_rows : (k + 1) * cold_rows, :]
        at += dr
    o_cold[...] = total


def scatter_body(cold_width, served, back, p_hot, o_hot, o_mid, o_cold, pad, hot_s, cold_s):
    step = pl.program_id(0)
    width = p_hot.shape[1]
    w_mid = o_mid.shape[1]
    slots = back.shape[0]

    @pl.when(step == 0)
    def _():
        cols = columns_of(served, pad)
        hot_s[...] = mm(back[:, 0:width], p_hot[...], NT).astype(BF16)
        lines = back[:, width + w_mid :]
        mine = lax.div(iota(lines.shape, 1), cold_width) == (cols[:, 2:3] & 3)
        cold_s[...] = jnp.where(mine, lines.astype(F32), 0.0).astype(BF16)

    def put(out, row, values):
        block = out.shape[0]
        hit = iota((block, slots), 0) + step * block == row
        out[...] = mm(ones_where(hit).astype(BF16), values)

    rows = served[0]
    put(o_hot, rows[0:1, :], hot_s[...])
    put(o_mid, rows[1:2, :], back[:, width : width + w_mid])
    put(o_cold, lax.shift_right_logical(rows[2:3, :], 2), cold_s[...])


def scatter_rows(serve_rows, back, proj_hot, shapes, cold_width):
    slots = serve_rows.shape[2]
    steps = 8

    def blocked(shape):
        return pl.BlockSpec((shape[0] // steps, shape[1]), lambda i: (i, 0))

    return pl.pallas_call(
        functools.partial(scatter_body, cold_width),
        grid=(steps,),
        out_shape=[sds(shape, F32) for shape in shapes],
        in_specs=[
            pl.BlockSpec(serve_rows.shape, lambda i: (0, 0, 0)),
            pl.BlockSpec(back.shape, lambda i: (0, 0)),
            pl.BlockSpec(proj_hot.shape, lambda i: (0, 0)),
        ],
        out_specs=[blocked(shape) for shape in shapes],
        scratch_shapes=[
            pltpu.VMEM((8, slots), jnp.int32),
            pltpu.VMEM((slots, shapes[0][1]), BF16),
            pltpu.VMEM((slots, shapes[2][1]), BF16),
        ],
        compiler_params=pltpu.CompilerParams(vmem_limit_bytes=24 * MIB),
        name="scatter_rows",
    )(serve_rows, back, proj_hot)


def local(
    groups,
    reps,
    table_hot,
    table_mid,
    table_cold,
    proj_hot,
    proj_mid,
    proj_cold,
    tower_in,
    tower_out,
    queries,
    labels,
    item_slot,
    item_block,
    serve_rows,
):
    devices = groups * reps
    slots = serve_rows.shape[2]
    cold_width, width = proj_cold.shape
    inner = tower_in.shape[1]
    items = item_slot.shape[2]
    nq = queries.shape[0]
    w_hot, w_mid, w_cold = table_hot.shape[1], table_mid.shape[1], table_cold.shape[1]
    raw_width = w_hot + w_mid + w_cold
    plan = Plan(groups, reps, width, inner, raw_width)

    def across_group(value, t):
        pairs = [(g * reps + r, (g ^ t) * reps + r) for g in range(groups) for r in range(reps)]
        return lax.ppermute(value, AXES, pairs)

    def across_rep(value, t):
        pairs = [(g * reps + r, g * reps + (r ^ t)) for g in range(groups) for r in range(reps)]
        return lax.ppermute(value, AXES, pairs)

    def to_all(rows):
        each = rows.reshape(devices, slots // devices, rows.shape[1])
        return lax.all_to_all(each, AXES, 0, 0, tiled=True).reshape(rows.shape)

    raw = to_all(gather_rows(serve_rows, table_hot, table_mid, table_cold, cold_width))
    label_row = labels.reshape(1, nq)
    q_all = [queries] + [across_group(queries, t) for t in range(1, groups)]
    l_all = [label_row] + [across_group(label_row, t) for t in range(1, groups)]
    by_item, by_slot = call(
        functools.partial(count_body, slots),
        [sds((items, 3 * slots), BF16), sds((3 * slots, items), BF16)],
        [item_slot, item_block],
        scratch=[pltpu.VMEM((8, items), jnp.int32)],
        name="counts",
    )
    blocks = groups * nq // QB
    pooled, resid, vec, stats = call(
        functools.partial(forward_body, groups),
        [
            sds((items, width), BF16),
            sds((items, width), F32),
            sds((items, width), BF16),
            sds((blocks, 3 * QB), F32),
        ],
        [raw, by_item, proj_hot, proj_mid, proj_cold, tower_in, tower_out] + q_all + l_all,
        scratch=[pltpu.VMEM((3 * slots, width), BF16)],
        vmem=48,
        name="forward",
    )
    s_all = [stats] + [across_group(stats, t) for t in range(1, groups)]
    cut_rows = plan.p1 + plan.p2
    loss, grad, keep, send, back = call(
        functools.partial(backward_body, plan, groups, F32),
        [
            sds((1, nq), F32),
            sds((items, groups * nq), BF16),
            sds((cut_rows, LANES), BF16),
            sds((cut_rows, LANES), BF16),
            sds((slots, width + w_mid + w_cold), BF16),
        ],
        s_all
        + q_all
        + l_all
        + [vec, resid, pooled, by_slot, raw, proj_hot, proj_mid, proj_cold, tower_in, tower_out],
        scratch=[
            pltpu.VMEM((8, LANES), F32),
            pltpu.VMEM((items, width), BF16),
            pltpu.VMEM((items, inner), BF16),
            pltpu.VMEM((items, inner), BF16),
            pltpu.VMEM((items, width), BF16),
            pltpu.VMEM((3 * slots, width), BF16),
            pltpu.VMEM((reps, plan.rows, LANES), BF16),
        ],
        vmem=56,
        name="backward",
    )
    back = to_all(back)

    got = across_group(send, 1)
    ky, kx, kz, m1, m2 = plan.ky, plan.kx, plan.kz, plan.m1, plan.m2

    def both(first, rows):
        return [(0, first), (1, first)], rows

    n1, n2 = plan.p1 // kx, plan.p2 // ky
    cuts = []
    for x in range(kx):
        cuts.append([(0, n1, [(0, x * n1), (1, x * n1)])])
    for y in range(ky):
        cuts.append([(0, n2, [(0, plan.p1 + y * n2), (1, plan.p1 + y * n2)])])
    parts = cut([keep, got], cuts, "sum_core")
    a_keep, a_send = parts[0], parts[1:kx]
    b_keep, b_send = parts[kx], parts[kx + 1 :]
    a_got = [across_rep(v, x + 1) for x, v in enumerate(a_send)]
    b_got = [across_group(v, 2 * (y + 1)) for y, v in enumerate(b_send)]
    k1, k2 = n1 // ky, n2 // kx
    na, nb = 1 + len(a_got), 1 + len(b_got)
    cuts = [[(0, k1, [(i, y * k1) for i in range(na)])] for y in range(ky)]
    cuts += [[(0, k2, [(na + i, x * k2) for i in range(nb)])] for x in range(kx)]
    parts = cut([a_keep, *a_got, b_keep, *b_got], cuts, "sum_xy")
    a_keep, a_send = parts[0], parts[1:ky]
    b_keep, b_send = parts[ky], parts[ky + 1 :]
    a_got = [across_group(v, 2 * (y + 1)) for y, v in enumerate(a_send)]
    b_got = [across_rep(v, x + 1) for x, v in enumerate(b_send)]
    na, nb = 1 + len(a_got), 1 + len(b_got)
    cuts = [
        [
            (0, m1, [(i, z * m1) for i in range(na)]),
            (m1, m2, [(na + i, z * m2) for i in range(nb)]),
        ]
        for z in range(kz)
    ]
    parts = cut([a_keep, *a_got, b_keep, *b_got], cuts, "sum_yx")
    z_got = [across_rep(parts[z], 2 * z) for z in range(1, kz)]
    mine = cut(
        [parts[0], *z_got], [[(0, m1 + m2, [(i, 0) for i in range(kz)])]], "sum_z"
    )[0]
    pieces = [mine] + [across_group(mine, t) for t in range(1, groups)]
    g_in, g_out, g_hot, g_mid, g_cold = call(
        functools.partial(final_body, plan, w_hot, w_mid, w_cold, cold_width),
        [
            sds((width, inner // reps), F32),
            sds((inner, width // reps), F32),
            sds((w_hot, width // reps), F32),
            sds((w_mid, width // reps), F32),
            sds((cold_width, width // reps), F32),
        ],
        pieces,
        scratch=[pltpu.VMEM((plan.rows, LANES), F32)],
        vmem=16,
        name="weights_out",
    )

    q_keep, q_send = call(
        functools.partial(query_grad_body, groups),
        [sds((groups // 2, width, nq), BF16), sds((groups // 2, width, nq), BF16)],
        [vec, grad],
        vmem=32,
        name="query_grad",
    )
    q_got = across_group(q_send, 1)
    own, *q_sends = call(
        query_core_body,
        [sds((width, nq), F32)] + [sds((width, nq), BF16)] * (ky - 1),
        [q_keep, q_got],
        vmem=16,
        name="query_core",
    )
    q_parts = [across_group(v, 2 * (y + 1)) for y, v in enumerate(q_sends)]
    query_grad = call(
        query_final_body, sds((nq, width), F32), [own, *q_parts], vmem=16, name="query_out"
    )

    o_hot, o_mid, o_cold = scatter_rows(
        serve_rows, back, proj_hot, [table_hot.shape, table_mid.shape, table_cold.shape], cold_width
    )
    return (
        loss.reshape(nq),
        query_grad,
        o_hot,
        o_mid,
        o_cold,
        g_hot,
        g_mid,
        g_cold,
        g_in,
        g_out,
    )


def solution(mesh):
    split = P(AXES, None)
    deep = P(AXES, None, None)
    return jax.shard_map(
        functools.partial(local, mesh.shape["group"], mesh.shape["rep"]),
        mesh=mesh,
        in_specs=(split, split, split, P(), P(), P(), P(), P(), split, P(AXES), deep, deep, deep),
        out_specs=(P(AXES), split, split, split, split) + (P(None, "rep"),) * 5,
        check_vma=False,
    )
```

```python
import functools

import jax
import jax.numpy as jnp
from jax import lax
from jax.experimental import pallas as pl
from jax.experimental.pallas import tpu as pltpu
from jax.sharding import PartitionSpec as P


NORM_EPS = 1e-06
LOGIT_SCALE = 0.2
LOG2_E = 1.4426950408889634
AXES = ("group", "rep")
LANES = 128
QB = 256
IB = 256
MIB = 1 << 20
F32 = jnp.float32
BF16 = jnp.bfloat16

NN = (((1,), (0,)), ((), ()))
NT = (((1,), (1,)), ((), ()))
TN = (((0,), (0,)), ((), ()))


def mm(left, right, dims=NN):
    return lax.dot_general(left, right, dims, preferred_element_type=F32)


def ones_where(mask):
    return jnp.where(mask, jnp.float32(1), jnp.float32(0))


def iota(shape, dim):
    return lax.broadcasted_iota(jnp.int32, shape, dim)


def call(body, out_shape, inputs, far=(), scratch=(), vmem=40):
    spec = pl.BlockSpec(memory_space=pltpu.VMEM)
    return pl.pallas_call(
        body,
        out_shape=out_shape,
        in_specs=[spec] * len(inputs) + [pl.BlockSpec(memory_space=pltpu.HBM)] * len(far),
        out_specs=jax.tree.map(lambda _: spec, out_shape),
        scratch_shapes=list(scratch),
        compiler_params=pltpu.CompilerParams(vmem_limit_bytes=vmem * MIB),
    )(*inputs, *far)


def sds(shape, dtype):
    return jax.ShapeDtypeStruct(shape, dtype)


def columns_of(served, pad_ref):
    pad_ref[...] = jnp.zeros_like(pad_ref)
    for k in range(served.shape[0]):
        pad_ref[k : k + 1, :] = served[k]
    return pad_ref[...].T


def parts_of(shape, lanes):
    return max(1, lanes // shape[1])


def split_row(row, part):
    return lax.div(row, part), lax.rem(row, part)


def gather_body(cold_width, served, hot, mid, cold, out, pad, v_hot, v_mid, v_cold, sems):
    copies = []
    sem = 0
    for table, wide in ((hot, v_hot), (mid, v_mid), (cold, v_cold)):
        part, w = wide.shape[0], table.shape[1]
        group = []
        for k in range(wide.shape[1] // w):
            copy = pltpu.make_async_copy(
                table.at[pl.ds(k * part, part), :],
                wide.at[:, pl.ds(k * w, w)],
                sems.at[sem],
            )
            sem += 1
            copy.start()
            group.append(copy)
        copies.append(group)
    idx = columns_of(served, pad)
    slots = out.shape[0]

    def pick(group, wide, row, w):
        part = wide.shape[0]
        which, low = split_row(row, part)
        hit = ones_where(iota((slots, part), 1) == low).astype(BF16)
        for copy in group:
            copy.wait()
        found = mm(hit, wide[...])
        value = found[:, 0:w]
        for k in range(1, wide.shape[1] // w):
            value = jnp.where(which == k, found[:, k * w : (k + 1) * w], value)
        return value

    w_hot, w_mid, w_cold = hot.shape[1], mid.shape[1], cold.shape[1]
    out[:, 0:w_hot] = pick(copies[0], v_hot, idx[:, 0:1], w_hot).astype(BF16)
    out[:, w_hot : w_hot + w_mid] = pick(copies[1], v_mid, idx[:, 1:2], w_mid).astype(BF16)
    row = idx[:, 2:3]
    lines = pick(copies[2], v_cold, lax.shift_right_logical(row, 2), w_cold)
    mine = lax.div(iota(lines.shape, 1), cold_width) == (row & 3)
    out[:, w_hot + w_mid :] = jnp.where(mine, lines, 0.0).astype(BF16)


def gather_rows(served, table_hot, table_mid, table_cold, cold_width):
    slots = served.shape[2]
    tables = (table_hot, table_mid, table_cold)
    width = sum(table.shape[1] for table in tables)
    lanes = max(table.shape[1] for table in tables)
    parts = [parts_of(table.shape, lanes) for table in tables]
    hbm = pl.BlockSpec(memory_space=pltpu.HBM)
    vmem = pl.BlockSpec(memory_space=pltpu.VMEM)
    return pl.pallas_call(
        functools.partial(gather_body, cold_width),
        out_shape=sds((slots, width), BF16),
        in_specs=[vmem, hbm, hbm, hbm],
        out_specs=vmem,
        scratch_shapes=[pltpu.VMEM((8, slots), jnp.int32)]
        + [
            pltpu.VMEM((t.shape[0] // p, t.shape[1] * p), BF16) for t, p in zip(tables, parts)
        ]
        + [pltpu.SemaphoreType.DMA((sum(parts),))],
        compiler_params=pltpu.CompilerParams(vmem_limit_bytes=60 * MIB),
        name="gather_rows",
    )(served, *tables)


def slot_of(slots, item_slot, item_block):
    return item_block[0] * slots + item_slot[0]


def count_body(slots, item_slot, item_block, by_item, pad):
    fields, items = item_slot.shape[1], item_slot.shape[2]
    pad[...] = jnp.zeros_like(pad)
    pad[0:fields, :] = slot_of(slots, item_slot, item_block)
    cols = pad[...].T
    for base in range(0, by_item.shape[1], QB):
        lanes = iota((items, QB), 1) + base
        total = jnp.zeros((items, QB), F32)
        for f in range(fields):
            total += ones_where(lanes == cols[:, f : f + 1])
        by_item[:, base : base + QB] = total.astype(BF16)


def count_slots(which, by_slot):
    for base in range(0, by_slot.shape[0], QB):
        rows = iota((QB, which.shape[1]), 0) + base
        total = jnp.zeros((QB, which.shape[1]), F32)
        for f in range(which.shape[0]):
            total += ones_where(rows == which[f : f + 1, :])
        by_slot[base : base + QB, :] = total.astype(BF16)


def tall(weight, times):
    return jnp.concatenate([weight] * times, axis=0)


def label_rows(label, base, jj):
    return label[0:1, jj * QB : (jj + 1) * QB] - base


def sigmoid(value):
    return 0.5 + 0.5 * jnp.tanh(0.5 * value)


def forward_body(peers, raw, p_hot, p_mid, p_cold, *rest):
    labels, far = rest[:peers], rest[peers : 2 * peers + 3]
    pooled_o, resid_o, vec_o, stats_o, exp_o, table = rest[2 * peers + 3 : 2 * peers + 9]
    near, sems = rest[2 * peers + 9 : -1], rest[-1]
    copies = [
        pltpu.make_async_copy(source, target, sems.at[k])
        for k, (source, target) in enumerate(zip(far, near))
    ]
    for copy in copies:
        copy.start()
    counts, t_in, t_out = near[:3]
    queries = near[3:]
    slots = raw.shape[0]
    w_hot, w_mid = p_hot.shape[0], p_mid.shape[0]
    w_cold = raw.shape[1] - w_hot - w_mid
    table[0:slots, :] = mm(raw[:, 0:w_hot], p_hot[...]).astype(BF16)
    table[slots : 2 * slots, :] = mm(raw[:, w_hot : w_hot + w_mid], p_mid[...]).astype(BF16)
    table[2 * slots :, :] = mm(
        raw[:, w_hot + w_mid :], tall(p_cold[...], w_cold // p_cold.shape[0])
    ).astype(BF16)
    items = counts.shape[0]
    for copy in copies[:3]:
        copy.wait()
    for at in range(0, items, IB):
        rows = slice(at, at + IB)
        pooled = mm(counts[rows, :], table[...]).astype(BF16)
        pre = mm(pooled, t_in[...])
        hidden = (pre * sigmoid(pre)).astype(BF16)
        resid = pooled.astype(F32) + mm(hidden, t_out[...])
        inv = lax.rsqrt(jnp.mean(resid * resid, axis=1, keepdims=True) + NORM_EPS)
        pooled_o[rows, :] = pooled
        resid_o[rows, :] = resid
        vec_o[rows, :] = (resid * inv).astype(BF16)
    base = lax.axis_index("group") * items
    per = queries[0].shape[0] // QB
    for t in range(peers):
        copies[3 + t].wait()
        for jj in range(per):
            s = mm(vec_o[...], queries[t][jj * QB : (jj + 1) * QB, :], NT)
            top = jnp.max(s, axis=0, keepdims=True)
            grown = jnp.exp2((s - top) * (LOGIT_SCALE * LOG2_E))
            total = jnp.sum(grown, axis=0, keepdims=True)
            hit = iota(s.shape, 0) == label_rows(labels[t], base, jj)
            picked = jnp.sum(jnp.where(hit, s, 0.0), axis=0, keepdims=True)
            j = t * per + jj
            exp_o[:, j * QB : (j + 1) * QB] = grown
            stats_o[j : j + 1, 0:QB] = LOGIT_SCALE * top
            stats_o[j : j + 1, QB : 2 * QB] = total
            stats_o[j : j + 1, 2 * QB :] = LOGIT_SCALE * picked


def slope_body(slots, item_slot, item_block, pooled, t_in, hidden_o, slope_o, by_slot):
    count_slots(slot_of(slots, item_slot, item_block), by_slot)
    for at in range(0, pooled.shape[0], IB):
        rows = slice(at, at + IB)
        pre = mm(pooled[rows, :], t_in[...])
        sig = sigmoid(pre)
        hidden_o[rows, :] = (pre * sig).astype(BF16)
        slope_o[rows, :] = sig * (1.0 + pre * (1.0 - sig))


class Plan:
    def __init__(self, groups, reps, width, inner, raw_width):
        self.groups, self.reps = groups, reps
        self.ky = groups // 2
        self.kx, self.kz = 2, reps // 2
        self.hr = inner // reps
        self.dr = width // reps
        self.b_in = width // LANES
        self.b_out = inner // LANES
        self.b_raw = raw_width // LANES
        rows = self.hr * self.b_in + self.dr * (self.b_out + self.b_raw)
        unit = 16 * self.ky
        units = -(-rows // (2 * unit))
        self.half = units * unit
        self.m1 = -(-units // 2) * 16
        self.m2 = units * 16 - self.m1
        self.rows = 2 * self.half
        self.used = rows
        self.p1 = reps * self.ky * self.m1
        self.p2 = reps * self.ky * self.m2


def backward_body(plan, peers, *refs):
    stats, refs = refs[:peers], refs[peers:]
    queries, refs = refs[:peers], refs[peers:]
    labels, refs = refs[:peers], refs[peers:]
    grown, hidden, slope, resid, pooled, by_slot, raw, p_hot, p_mid, p_cold, t_in, t_out = refs[:12]
    loss_o, grad_o, keep_o, send_o, back_o = refs[12:17]
    low_s, pre_s, pgrad_s, slot_s, chunk = refs[17:]
    items, width = pooled.shape
    nq = queries[0].shape[0]
    per = nq // QB
    me_g, me_r = lax.axis_index("group"), lax.axis_index("rep")
    base = me_g * items
    for t in range(peers):
        for jj in range(per):
            rows = [(t ^ s) * per + jj for s in range(peers)]
            tops = [stats[s][rows[s] : rows[s] + 1, 0:QB] for s in range(peers)]
            totals = [stats[s][rows[s] : rows[s] + 1, QB : 2 * QB] for s in range(peers)]
            top = functools.reduce(jnp.maximum, tops)
            total = sum(tot * jnp.exp(m - top) for m, tot in zip(tops, totals))
            log_total = top + jnp.log(total)
            if t == 0:
                picked = sum(stats[s][rows[s] : rows[s] + 1, 2 * QB :] for s in range(peers))
                loss_o[0:1, jj * QB : (jj + 1) * QB] = log_total - picked
            at = t * nq + jj * QB
            share = grown[:, at : at + QB] * jnp.exp(tops[0] - log_total)
            hit = iota(share.shape, 0) == label_rows(labels[t], base, jj)
            grad_o[:, at : at + QB] = (share - ones_where(hit)).astype(BF16)
    for at in range(0, items, IB):
        rows = slice(at, at + IB)
        vgrad = mm(grad_o[rows, 0:nq], queries[0][...])
        for t in range(1, peers):
            vgrad += mm(grad_o[rows, t * nq : (t + 1) * nq], queries[t][...])
        vgrad = LOGIT_SCALE * vgrad
        res = resid[rows, :]
        inv = lax.rsqrt(jnp.mean(res * res, axis=1, keepdims=True) + NORM_EPS)
        dot_wide = jnp.sum(vgrad * res, axis=1, keepdims=True)
        wide = inv * vgrad - (inv * inv * inv / width * dot_wide) * res
        low = wide.astype(BF16)
        low_s[rows, :] = low
        pre_g = (mm(low, t_out[...], NT) * slope[rows, :]).astype(BF16)
        pre_s[rows, :] = pre_g
        pgrad_s[rows, :] = (mm(pre_g, t_in[...], NT) + wide).astype(BF16)
    slots = raw.shape[0]
    w_hot, w_mid = p_hot.shape[0], p_mid.shape[0]
    w_cold = raw.shape[1] - w_hot - w_mid
    slot_s[...] = mm(by_slot[...], pgrad_s[...]).astype(BF16)
    back_o[:, 0:width] = slot_s[0:slots, :]
    back_o[:, width : width + w_mid] = mm(slot_s[slots : 2 * slots, :], p_mid[...], NT).astype(BF16)
    back_o[:, width + w_mid :] = mm(
        slot_s[2 * slots :, :], tall(p_cold[...], w_cold // p_cold.shape[0]), NT
    ).astype(BF16)

    g_in = mm(pooled[...], pre_s[...], TN).T
    hr, dr = plan.hr, plan.dr
    for r in range(plan.reps):
        for b in range(plan.b_in):
            chunk[r, b * hr : (b + 1) * hr, :] = g_in[
                r * hr : (r + 1) * hr, b * LANES : (b + 1) * LANES
            ].astype(BF16)
    at = hr * plan.b_in
    g_out = mm(low_s[...], hidden[...], TN)
    parts = [(g_out, plan.b_out)]
    lane = 0
    for b, w in enumerate((w_hot, w_mid, w_cold)):
        parts.append(
            (mm(slot_s[b * slots : (b + 1) * slots, :], raw[:, lane : lane + w], TN), w // LANES)
        )
        lane += w
    for value, blocks in parts:
        for r in range(plan.reps):
            for b in range(blocks):
                chunk[r, at + b * dr : at + (b + 1) * dr, :] = value[
                    r * dr : (r + 1) * dr, b * LANES : (b + 1) * LANES
                ].astype(BF16)
        at += blocks * dr
    if plan.rows > plan.used:
        chunk[:, plan.used :, :] = jnp.zeros((plan.reps, plan.rows - plan.used, LANES), BF16)
    core, me_y = me_g & 1, lax.shift_right_logical(me_g, 1)
    for h, out in ((0, keep_o), (1, send_o)):
        start = (core ^ h) * plan.half
        for z in range(plan.kz):
            for x in range(plan.kx):
                r = me_r ^ (z * 2 + x)
                for y in range(plan.ky):
                    q = me_y ^ y
                    m = plan.m1
                    at = ((x * plan.ky + y) * plan.kz + z) * m
                    row = pl.multiple_of(start + q * m, 16)
                    out[at : at + m, :] = chunk[r, pl.ds(row, m), :]
                    m = plan.m2
                    if m:
                        at = plan.p1 + ((y * plan.kx + x) * plan.kz + z) * m
                        row = pl.multiple_of(start + plan.ky * plan.m1 + q * m, 16)
                        out[at : at + m, :] = chunk[r, pl.ds(row, m), :]


def query_grad_body(peers, vec, grad, keep_o, send_o):
    turned = vec[...].T
    nq = keep_o.shape[2]
    for t in range(peers):
        part = (LOGIT_SCALE * mm(turned, grad[:, t * nq : (t + 1) * nq])).astype(BF16)
        (send_o if t & 1 else keep_o)[t // 2] = part


def query_core_body(keep, got, own_o, *sends):
    own_o[...] = keep[0].astype(F32) + got[0].astype(F32)
    for y, out in enumerate(sends):
        out[...] = (keep[y + 1].astype(F32) + got[y + 1].astype(F32)).astype(BF16)


def query_final_body(own, *rest):
    got, out = rest[:-1], rest[-1]
    total = own[...]
    for part in got:
        total += part[...].astype(F32)
    out[...] = total.T


def cut_body(cuts, *refs):
    n_in = len(refs) - len(cuts)
    for out, pieces in zip(refs[n_in:], cuts):
        for at, rows, terms in pieces:
            total = None
            for i, first in terms:
                part = refs[i][first : first + rows, :].astype(F32)
                total = part if total is None else total + part
            out[at : at + rows, :] = total.astype(out.dtype)


def cut(inputs, cuts):
    shapes = [sds((sum(p[1] for p in pieces), LANES), BF16) for pieces in cuts]
    return call(functools.partial(cut_body, cuts), shapes, inputs, vmem=8)


def final_body(plan, w_hot, w_mid, w_cold, cold_rows, *refs):
    pieces = refs[: plan.groups]
    o_in, o_out, o_hot, o_mid, o_cold, chunk = refs[plan.groups :]
    me_g = lax.axis_index("group")
    for t in range(plan.groups):
        h = (me_g & 1) ^ (t & 1)
        q = lax.shift_right_logical(me_g, 1) ^ (t >> 1)
        start = h * plan.half
        row = pl.multiple_of(start + q * plan.m1, 16)
        chunk[pl.ds(row, plan.m1), :] = pieces[t][0 : plan.m1, :].astype(F32)
        if plan.m2:
            row = pl.multiple_of(start + plan.ky * plan.m1 + q * plan.m2, 16)
            chunk[pl.ds(row, plan.m2), :] = pieces[t][plan.m1 :, :].astype(F32)
    hr, dr = plan.hr, plan.dr
    for b in range(plan.b_in):
        o_in[b * LANES : (b + 1) * LANES, :] = chunk[b * hr : (b + 1) * hr, :].T
    at = hr * plan.b_in
    for out, w in ((o_out, plan.b_out * LANES), (o_hot, w_hot), (o_mid, w_mid)):
        for b in range(w // LANES):
            out[:, b * LANES : (b + 1) * LANES] = chunk[at : at + dr, :]
            at += dr
    total = jnp.zeros((cold_rows, dr), F32)
    for _ in range(w_cold // LANES):
        turned = chunk[at : at + dr, :].T
        for k in range(LANES // cold_rows):
            total += turned[k * cold_rows : (k + 1) * cold_rows, :]
        at += dr
    o_cold[...] = total


def scatter_body(cold_width, served, back, p_hot, o_hot, o_mid, o_cold, pad, s_hot, s_mid, s_cold):
    step = pl.program_id(0)
    steps = pl.num_programs(0)
    width = p_hot.shape[1]
    slots = back.shape[0]
    w_mid = o_mid.shape[2]

    @pl.when(step == 0)
    def _():
        cols = columns_of(served, pad)
        s_hot[...] = mm(back[:, 0:width], p_hot[...], NT).astype(BF16)

        def widen(wide, row, part, values):
            w = values.shape[1]
            which = split_row(row, part)[0]
            for k in range(wide.shape[1] // w):
                wide[:, k * w : (k + 1) * w] = jnp.where(which == k, values, 0.0).astype(BF16)

        mids = back[:, width : width + w_mid].astype(F32)
        widen(s_mid, cols[:, 1:2], o_mid.shape[1] * steps, mids)
        lines = back[:, width + w_mid :].astype(F32)
        mine = lax.div(iota(lines.shape, 1), cold_width) == (cols[:, 2:3] & 3)
        row = lax.shift_right_logical(cols[:, 2:3], 2)
        widen(s_cold, row, o_cold.shape[1] * steps, jnp.where(mine, lines, 0.0))

    def put(out, row, wide):
        block, w = out.shape[1], out.shape[2]
        low = split_row(row, block * steps)[1]
        hit = ones_where(iota((block, slots), 0) + step * block == low).astype(BF16)
        found = mm(hit, wide[...])
        for k in range(out.shape[0]):
            out[k] = found[:, k * w : (k + 1) * w]

    put(o_hot, served[0], s_hot)
    put(o_mid, served[1], s_mid)
    put(o_cold, lax.shift_right_logical(served[2], 2), s_cold)


def scatter_rows(served, back, proj_hot, shapes, cold_width):
    slots = served.shape[2]
    steps = 8
    lanes = max(shape[1] for shape in shapes)
    wide = [(parts_of(shape, lanes), shape) for shape in shapes]
    outs = [(p, shape[0] // p, shape[1]) for p, shape in wide]
    found = pl.pallas_call(
        functools.partial(scatter_body, cold_width),
        grid=(steps,),
        out_shape=[sds(shape, F32) for shape in outs],
        in_specs=[
            pl.BlockSpec(served.shape, lambda i: (0, 0, 0)),
            pl.BlockSpec(back.shape, lambda i: (0, 0)),
            pl.BlockSpec(proj_hot.shape, lambda i: (0, 0)),
        ],
        out_specs=[
            pl.BlockSpec((p, rows // steps, w), lambda i: (0, i, 0)) for p, rows, w in outs
        ],
        scratch_shapes=[pltpu.VMEM((8, slots), jnp.int32)]
        + [pltpu.VMEM((slots, p * w), BF16) for p, _, w in outs],
        compiler_params=pltpu.CompilerParams(vmem_limit_bytes=12 * MIB),
        name="scatter_rows",
    )(served, back, proj_hot)
    return [value.reshape(shape) for value, shape in zip(found, shapes)]


def local(
    groups,
    reps,
    table_hot,
    table_mid,
    table_cold,
    proj_hot,
    proj_mid,
    proj_cold,
    tower_in,
    tower_out,
    queries,
    labels,
    item_slot,
    item_block,
    serve_rows,
):
    devices = groups * reps
    slots = serve_rows.shape[2]
    cold_width, width = proj_cold.shape
    inner = tower_in.shape[1]
    items = item_slot.shape[2]
    nq = queries.shape[0]
    w_hot, w_mid, w_cold = table_hot.shape[1], table_mid.shape[1], table_cold.shape[1]
    raw_width = w_hot + w_mid + w_cold
    plan = Plan(groups, reps, width, inner, raw_width)

    def across_group(value, t):
        pairs = [(g * reps + r, (g ^ t) * reps + r) for g in range(groups) for r in range(reps)]
        return lax.ppermute(value, AXES, pairs)

    def across_rep(value, t):
        pairs = [(g * reps + r, g * reps + (r ^ t)) for g in range(groups) for r in range(reps)]
        return lax.ppermute(value, AXES, pairs)

    def to_all(rows):
        each = rows.reshape(devices, slots // devices, rows.shape[1])
        return lax.all_to_all(each, AXES, 0, 0, tiled=True).reshape(rows.shape)

    def to_group(value):
        found = {0: value}
        for t in range(2, groups, 2):
            found[t] = across_group(value, t)
        for t in range(0, groups, 2):
            found[t + 1] = across_group(found[t], 1)
        return [found[t] for t in range(groups)]

    served = jnp.transpose(serve_rows, (1, 0, 2))
    q_all = to_group(queries)
    rows = gather_rows(served, table_hot, table_mid, table_cold, cold_width)
    raw = to_all(rows)
    l_all = to_group(labels.reshape(1, nq))
    by_item = call(
        functools.partial(count_body, slots),
        sds((items, 3 * slots), BF16),
        [item_slot, item_block],
        scratch=[pltpu.VMEM((8, items), jnp.int32)],
        vmem=60,
    )
    blocks = groups * nq // QB
    far = [by_item, tower_in, tower_out] + q_all
    pooled, resid, vec, stats, grown = call(
        functools.partial(forward_body, groups),
        [
            sds((items, width), BF16),
            sds((items, width), F32),
            sds((items, width), BF16),
            sds((blocks, 3 * QB), F32),
            sds((items, groups * nq), F32),
        ],
        [raw, proj_hot, proj_mid, proj_cold] + l_all,
        far,
        scratch=[pltpu.VMEM((3 * slots, width), BF16)]
        + [pltpu.VMEM(value.shape, value.dtype) for value in far]
        + [pltpu.SemaphoreType.DMA((len(far),))],
        vmem=26 + 2 * groups,
    )
    s_all = [stats]
    for t in range(1, groups):
        s_all.append(across_group(stats, t))
    hidden, slope, by_slot = call(
        functools.partial(slope_body, slots),
        [sds((items, inner), BF16), sds((items, inner), F32), sds((3 * slots, items), BF16)],
        [item_slot, item_block, pooled, tower_in],
        vmem=12,
    )
    cut_rows = plan.p1 + plan.p2
    loss, grad, keep, send, back = call(
        functools.partial(backward_body, plan, groups),
        [
            sds((1, nq), F32),
            sds((items, groups * nq), BF16),
            sds((cut_rows, LANES), BF16),
            sds((cut_rows, LANES), BF16),
            sds((slots, width + w_mid + w_cold), BF16),
        ],
        s_all
        + q_all
        + l_all
        + [grown, hidden, slope, resid, pooled, by_slot, raw]
        + [proj_hot, proj_mid, proj_cold, tower_in, tower_out],
        scratch=[
            pltpu.VMEM((items, width), BF16),
            pltpu.VMEM((items, inner), BF16),
            pltpu.VMEM((items, width), BF16),
            pltpu.VMEM((3 * slots, width), BF16),
            pltpu.VMEM((reps, plan.rows, LANES), BF16),
        ],
        vmem=8 * groups - 8,
    )
    back = to_all(back)

    got = across_group(send, 1)
    ky, kx, kz, m1, m2 = plan.ky, plan.kx, plan.kz, plan.m1, plan.m2

    n1, n2 = plan.p1 // kx, plan.p2 // ky
    cuts = []
    for x in range(kx):
        cuts.append([(0, n1, [(0, x * n1), (1, x * n1)])])
    for y in range(ky):
        cuts.append([(0, n2, [(0, plan.p1 + y * n2), (1, plan.p1 + y * n2)])])
    parts = cut([keep, got], cuts)
    a_keep, a_send = parts[0], parts[1:kx]
    b_keep, b_send = parts[kx], parts[kx + 1 :]
    a_got = [across_rep(v, x + 1) for x, v in enumerate(a_send)]
    b_got = [across_group(v, 2 * (y + 1)) for y, v in enumerate(b_send)]
    k1, k2 = n1 // ky, n2 // kx
    na, nb = 1 + len(a_got), 1 + len(b_got)
    cuts = [[(0, k1, [(i, y * k1) for i in range(na)])] for y in range(ky)]
    cuts += [[(0, k2, [(na + i, x * k2) for i in range(nb)])] for x in range(kx)]
    parts = cut([a_keep, *a_got, b_keep, *b_got], cuts)
    a_keep, a_send = parts[0], parts[1:ky]
    b_keep, b_send = parts[ky], parts[ky + 1 :]
    a_got = [across_group(v, 2 * (y + 1)) for y, v in enumerate(a_send)]
    b_got = [across_rep(v, x + 1) for x, v in enumerate(b_send)]
    na, nb = 1 + len(a_got), 1 + len(b_got)
    cuts = [
        [
            (0, m1, [(i, z * m1) for i in range(na)]),
            (m1, m2, [(na + i, z * m2) for i in range(nb)]),
        ]
        for z in range(kz)
    ]
    parts = cut([a_keep, *a_got, b_keep, *b_got], cuts)
    z_got = [across_rep(parts[z], 2 * z) for z in range(1, kz)]
    mine = cut([parts[0], *z_got], [[(0, m1 + m2, [(i, 0) for i in range(kz)])]])[0]
    pieces = [mine] + [across_group(mine, t) for t in range(1, groups)]
    g_in, g_out, g_hot, g_mid, g_cold = call(
        functools.partial(final_body, plan, w_hot, w_mid, w_cold, cold_width),
        [
            sds((width, inner // reps), F32),
            sds((width // reps, inner), F32),
            sds((width // reps, w_hot), F32),
            sds((width // reps, w_mid), F32),
            sds((cold_width, width // reps), F32),
        ],
        pieces,
        scratch=[pltpu.VMEM((plan.rows, LANES), F32)],
        vmem=16,
    )

    q_keep, q_send = call(
        functools.partial(query_grad_body, groups),
        [sds((groups // 2, width, nq), BF16), sds((groups // 2, width, nq), BF16)],
        [vec, grad],
        vmem=16,
    )
    q_got = across_group(q_send, 1)
    own, *q_sends = call(
        query_core_body,
        [sds((width, nq), F32)] + [sds((width, nq), BF16)] * (ky - 1),
        [q_keep, q_got],
        vmem=16,
    )
    q_parts = [across_group(v, 2 * (y + 1)) for y, v in enumerate(q_sends)]
    query_grad = call(query_final_body, sds((nq, width), F32), [own, *q_parts], vmem=8)
    shapes = [table_hot.shape, table_mid.shape, table_cold.shape]
    o_hot, o_mid, o_cold = scatter_rows(served, back, proj_hot, shapes, cold_width)
    return (
        loss.reshape(nq),
        query_grad,
        o_hot,
        o_mid,
        o_cold,
        g_hot.T,
        g_mid.T,
        g_cold,
        g_in,
        g_out.T,
    )


def solution(mesh):
    split = P(AXES, None)
    deep = P(AXES, None, None)

    def body(*args):
        return local(mesh.shape["group"], mesh.shape["rep"], *args)

    return jax.shard_map(
        body,
        mesh=mesh,
        in_specs=(split, split, split, P(), P(), P(), P(), P(), split, P(AXES), deep, deep, deep),
        out_specs=(P(AXES), split, split, split, split) + (P(None, "rep"),) * 5,
        check_vma=False,
    )
```

```python
import functools

import jax
import jax.numpy as jnp
from jax import lax
from jax.experimental import pallas as pl
from jax.experimental.pallas import tpu as pltpu
from jax.sharding import PartitionSpec as P


NORM_EPS = 1e-06
LOGIT_SCALE = 0.2
LOG2_E = 1.4426950408889634
AXES = ("group", "rep")
LANES = 128
QB = 256
IB = 256
MIB = 1 << 20
F32 = jnp.float32
BF16 = jnp.bfloat16

NN = (((1,), (0,)), ((), ()))
NT = (((1,), (1,)), ((), ()))
TN = (((0,), (0,)), ((), ()))


def mm(left, right, dims=NN):
    return lax.dot_general(left, right, dims, preferred_element_type=F32)


def ones_where(mask):
    return jnp.where(mask, jnp.float32(1), jnp.float32(0))


def iota(shape, dim):
    return lax.broadcasted_iota(jnp.int32, shape, dim)


def call(body, out_shape, inputs, far=(), scratch=(), vmem=40):
    spec = pl.BlockSpec(memory_space=pltpu.VMEM)
    return pl.pallas_call(
        body,
        out_shape=out_shape,
        in_specs=[spec] * len(inputs) + [pl.BlockSpec(memory_space=pltpu.HBM)] * len(far),
        out_specs=jax.tree.map(lambda _: spec, out_shape),
        scratch_shapes=list(scratch),
        compiler_params=pltpu.CompilerParams(vmem_limit_bytes=vmem * MIB),
    )(*inputs, *far)


def sds(shape, dtype):
    return jax.ShapeDtypeStruct(shape, dtype)


def columns_of(served, pad_ref):
    pad_ref[...] = jnp.zeros_like(pad_ref)
    for k in range(served.shape[0]):
        pad_ref[k : k + 1, :] = served[k]
    return pad_ref[...].T


def parts_of(shape, lanes):
    return max(1, lanes // shape[1])


def split_row(row, part):
    return lax.div(row, part), lax.rem(row, part)


def gather_body(cold_width, parts, served, hot, mid, cold, out, pad, asked, v_hot, v_mid, v_cold, sems):
    copies = [
        pltpu.make_async_copy(source, target, sems.at[k])
        for k, (source, target) in enumerate(
            ((served, asked), (hot, v_hot), (mid, v_mid), (cold, v_cold))
        )
    ]
    for copy in copies:
        copy.start()
    copies[0].wait()
    idx = columns_of(asked, pad)
    slots = out.shape[0]

    def pick(k, table, row, w):
        part = table.shape[0] // parts[k]
        which, low = split_row(row, part)
        hit = ones_where(iota((slots, part), 1) == low).astype(BF16)
        copies[k + 1].wait()
        wide = [table[p * part : (p + 1) * part, :] for p in range(parts[k])]
        found = mm(hit, wide[0] if parts[k] == 1 else jnp.concatenate(wide, axis=1))
        value = found[:, 0:w]
        for p in range(1, parts[k]):
            value = jnp.where(which == p, found[:, p * w : (p + 1) * w], value)
        return value

    w_hot, w_mid, w_cold = hot.shape[1], mid.shape[1], cold.shape[1]
    out[:, 0:w_hot] = pick(0, v_hot, idx[:, 0:1], w_hot).astype(BF16)
    out[:, w_hot : w_hot + w_mid] = pick(1, v_mid, idx[:, 1:2], w_mid).astype(BF16)
    row = idx[:, 2:3]
    lines = pick(2, v_cold, lax.shift_right_logical(row, 2), w_cold)
    mine = lax.div(iota(lines.shape, 1), cold_width) == (row & 3)
    out[:, w_hot + w_mid :] = jnp.where(mine, lines, 0.0).astype(BF16)


def gather_rows(served, table_hot, table_mid, table_cold, cold_width):
    slots = served.shape[2]
    tables = (table_hot, table_mid, table_cold)
    width = sum(table.shape[1] for table in tables)
    lanes = max(table.shape[1] for table in tables)
    parts = [parts_of(table.shape, lanes) for table in tables]
    hbm = pl.BlockSpec(memory_space=pltpu.HBM)
    vmem = pl.BlockSpec(memory_space=pltpu.VMEM)
    return pl.pallas_call(
        functools.partial(gather_body, cold_width, parts),
        out_shape=sds((slots, width), BF16),
        in_specs=[hbm, hbm, hbm, hbm],
        out_specs=vmem,
        scratch_shapes=[pltpu.VMEM((8, slots), jnp.int32), pltpu.VMEM(served.shape, jnp.int32)]
        + [pltpu.VMEM(table.shape, BF16) for table in tables]
        + [pltpu.SemaphoreType.DMA((4,))],
        compiler_params=pltpu.CompilerParams(vmem_limit_bytes=60 * MIB),
        name="gather_rows",
    )(served, *tables)


def slot_of(slots, item_slot, item_block):
    return item_block[0] * slots + item_slot[0]


def count_body(slots, item_slot, item_block, by_item, by_slot, pad):
    fields, items = item_slot.shape[1], item_slot.shape[2]
    which = slot_of(slots, item_slot, item_block)
    count_slots(which, by_slot)
    pad[...] = jnp.zeros_like(pad)
    pad[0:fields, :] = which
    cols = pad[...].T
    for base in range(0, by_item.shape[1], QB):
        lanes = iota((items, QB), 1) + base
        total = jnp.zeros((items, QB), F32)
        for f in range(fields):
            total += ones_where(lanes == cols[:, f : f + 1])
        by_item[:, base : base + QB] = total.astype(BF16)


def count_slots(which, by_slot):
    for base in range(0, by_slot.shape[0], QB):
        rows = iota((QB, which.shape[1]), 0) + base
        total = jnp.zeros((QB, which.shape[1]), F32)
        for f in range(which.shape[0]):
            total += ones_where(rows == which[f : f + 1, :])
        by_slot[base : base + QB, :] = total.astype(BF16)


def tall(weight, times):
    return jnp.concatenate([weight] * times, axis=0)


def label_rows(label, base, jj):
    row = label[0:1, jj * QB : (jj + 1) * QB] - base
    return row - iota((8, QB), 0)


def hits(rows, label, at):
    first = 8 * iota((rows // 8, 8, QB), 0) + at
    return first == label[None]


def by_eight(value):
    return value.reshape(value.shape[0] // 8, 8, value.shape[1])


def sigmoid(value):
    return 0.5 + 0.5 * jnp.tanh(0.5 * value)


def forward_body(peers, raw, counts, p_hot, p_mid, p_cold, t_in, t_out, *rest):
    queries, labels = rest[:peers], rest[peers : 2 * peers]
    pooled_o, resid_o, vec_o, stats_o, tops_o, exp_o, table = rest[2 * peers :]
    slots = raw.shape[0]
    w_hot, w_mid = p_hot.shape[0], p_mid.shape[0]
    w_cold = raw.shape[1] - w_hot - w_mid
    table[0:slots, :] = mm(raw[:, 0:w_hot], p_hot[...]).astype(BF16)
    table[slots : 2 * slots, :] = mm(raw[:, w_hot : w_hot + w_mid], p_mid[...]).astype(BF16)
    table[2 * slots :, :] = mm(
        raw[:, w_hot + w_mid :], tall(p_cold[...], w_cold // p_cold.shape[0])
    ).astype(BF16)
    items = counts.shape[0]
    base = lax.axis_index("group") * items
    nq = queries[0].shape[0]
    per = nq // QB
    blocks = [(t, jj) for t in range(peers) for jj in range(per)]
    wanted = [label_rows(labels[t], base, jj) for t, jj in blocks]
    kept = [[] for _ in blocks]
    step = t_in.shape[1] // 4

    def tower(ib):
        rows = slice(ib * IB, (ib + 1) * IB)
        pooled = mm(counts[rows, :], table[...]).astype(BF16)
        pooled_o[rows, :] = pooled
        resid = pooled.astype(F32)
        yield
        for at in range(0, t_in.shape[1], step):
            pre = mm(pooled, t_in[:, at : at + step])
            hidden = (pre * sigmoid(pre)).astype(BF16)
            yield
            resid += mm(hidden, t_out[at : at + step, :])
        inv = lax.rsqrt(jnp.mean(resid * resid, axis=1, keepdims=True) + NORM_EPS)
        resid_o[rows, :] = resid
        vec_o[rows, :] = (resid * inv).astype(BF16)

    def score(ib, j):
        at = ib * IB
        rows = slice(at, at + IB)
        t, jj = blocks[j]
        s = mm(vec_o[rows, :], queries[t][jj * QB : (jj + 1) * QB, :], NT)
        top = jnp.max(s, axis=0, keepdims=True)
        grown = jnp.exp2((s - top) * (LOGIT_SCALE * LOG2_E))
        total = jnp.sum(grown, axis=0, keepdims=True)
        picked = jnp.where(hits(IB, wanted[j], at), by_eight(s), 0.0)
        picked = jnp.sum(jnp.sum(picked, axis=0), axis=0, keepdims=True)
        exp_o[rows, j * QB : (j + 1) * QB] = grown
        top = LOGIT_SCALE * top
        tops_o[j : j + 1, ib * QB : (ib + 1) * QB] = top
        kept[j].append((top, total, LOGIT_SCALE * picked))

    for _ in tower(0):
        pass
    for ib in range(items // IB):
        ahead = tower(ib + 1) if ib + 1 < items // IB else iter(())
        for j in range(len(blocks)):
            next(ahead, None)
            score(ib, j)
        for _ in ahead:
            pass
    for j, parts in enumerate(kept):
        top = functools.reduce(jnp.maximum, [part[0] for part in parts])
        stats_o[j : j + 1, 0:QB] = top
        stats_o[j : j + 1, QB : 2 * QB] = sum(p[1] * jnp.exp(p[0] - top) for p in parts)
        stats_o[j : j + 1, 2 * QB :] = sum(part[2] for part in parts)


def slope_body(pooled, t_in, hidden_o, slope_o):
    for at in range(0, pooled.shape[0], IB):
        rows = slice(at, at + IB)
        pre = mm(pooled[rows, :], t_in[...])
        sig = sigmoid(pre)
        hidden_o[rows, :] = (pre * sig).astype(BF16)
        slope_o[rows, :] = sig * (1.0 + pre * (1.0 - sig))


class Plan:
    def __init__(self, groups, reps, width, inner, raw_width):
        self.groups, self.reps = groups, reps
        self.ky = groups // 2
        self.kx, self.kz = 2, reps // 2
        self.hr = inner // reps
        self.dr = width // reps
        self.b_in = width // LANES
        self.b_out = inner // LANES
        self.b_raw = raw_width // LANES
        rows = self.hr * self.b_in + self.dr * (self.b_out + self.b_raw)
        unit = 16 * self.ky
        units = -(-rows // (2 * unit))
        self.half = units * unit
        self.m1 = -(-units // 2) * 16
        self.m2 = units * 16 - self.m1
        self.rows = 2 * self.half
        self.used = rows
        self.p1 = reps * self.ky * self.m1
        self.p2 = reps * self.ky * self.m2


def backward_body(plan, peers, *refs):
    stats, refs = refs[:peers], refs[peers:]
    queries, refs = refs[:peers], refs[peers:]
    labels, refs = refs[:peers], refs[peers:]
    tops_r, grown, hidden, slope, resid, pooled, by_slot, raw = refs[:8]
    p_hot, p_mid, p_cold, t_in, t_out = refs[8:13]
    loss_o, grad_o, keep_o, send_o, back_o = refs[13:18]
    low_s, pre_s, pgrad_s, slot_s, chunk = refs[18:]
    items, width = pooled.shape
    nq = queries[0].shape[0]
    per = nq // QB
    me_g, me_r = lax.axis_index("group"), lax.axis_index("rep")
    base = me_g * items
    log_totals, wanted = [], []
    for t in range(peers):
        for jj in range(per):
            rows = [(t ^ s) * per + jj for s in range(peers)]
            tops = [stats[s][rows[s] : rows[s] + 1, 0:QB] for s in range(peers)]
            totals = [stats[s][rows[s] : rows[s] + 1, QB : 2 * QB] for s in range(peers)]
            top = functools.reduce(jnp.maximum, tops)
            total = sum(tot * jnp.exp(m - top) for m, tot in zip(tops, totals))
            log_total = top + jnp.log(total)
            if t == 0:
                picked = sum(stats[s][rows[s] : rows[s] + 1, 2 * QB :] for s in range(peers))
                loss_o[0:1, jj * QB : (jj + 1) * QB] = log_total - picked
            log_totals.append(log_total)
            wanted.append(label_rows(labels[t], base, jj))
    for at in range(0, items, IB):
        rows = slice(at, at + IB)
        for j, log_total in enumerate(log_totals):
            ib = at // IB
            scale = jnp.exp(tops_r[j : j + 1, ib * QB : (ib + 1) * QB] - log_total)
            share = by_eight(grown[rows, j * QB : (j + 1) * QB] * scale)
            share = share - ones_where(hits(IB, wanted[j], at))
            grad_o[rows, j * QB : (j + 1) * QB] = share.reshape(IB, QB).astype(BF16)
        vgrad = mm(grad_o[rows, 0:nq], queries[0][...])
        for t in range(1, peers):
            vgrad += mm(grad_o[rows, t * nq : (t + 1) * nq], queries[t][...])
        vgrad = LOGIT_SCALE * vgrad
        res = resid[rows, :]
        inv = lax.rsqrt(jnp.mean(res * res, axis=1, keepdims=True) + NORM_EPS)
        dot_wide = jnp.sum(vgrad * res, axis=1, keepdims=True)
        wide = inv * vgrad - (inv * inv * inv / width * dot_wide) * res
        low = wide.astype(BF16)
        low_s[rows, :] = low
        pre_g = (mm(low, t_out[...], NT) * slope[rows, :]).astype(BF16)
        pre_s[rows, :] = pre_g
        pgrad_s[rows, :] = (mm(pre_g, t_in[...], NT) + wide).astype(BF16)
    slots = raw.shape[0]
    w_hot, w_mid = p_hot.shape[0], p_mid.shape[0]
    w_cold = raw.shape[1] - w_hot - w_mid
    slot_s[...] = mm(by_slot[...], pgrad_s[...]).astype(BF16)
    back_o[:, 0:width] = slot_s[0:slots, :]
    back_o[:, width : width + w_mid] = mm(slot_s[slots : 2 * slots, :], p_mid[...], NT).astype(BF16)
    back_o[:, width + w_mid :] = mm(
        slot_s[2 * slots :, :], tall(p_cold[...], w_cold // p_cold.shape[0]), NT
    ).astype(BF16)

    g_in = mm(pooled[...], pre_s[...], TN).T
    hr, dr = plan.hr, plan.dr
    for r in range(plan.reps):
        for b in range(plan.b_in):
            chunk[r, b * hr : (b + 1) * hr, :] = g_in[
                r * hr : (r + 1) * hr, b * LANES : (b + 1) * LANES
            ].astype(BF16)
    at = hr * plan.b_in
    g_out = mm(low_s[...], hidden[...], TN)
    parts = [(g_out, plan.b_out)]
    lane = 0
    for b, w in enumerate((w_hot, w_mid, w_cold)):
        parts.append(
            (mm(slot_s[b * slots : (b + 1) * slots, :], raw[:, lane : lane + w], TN), w // LANES)
        )
        lane += w
    for value, blocks in parts:
        for r in range(plan.reps):
            for b in range(blocks):
                chunk[r, at + b * dr : at + (b + 1) * dr, :] = value[
                    r * dr : (r + 1) * dr, b * LANES : (b + 1) * LANES
                ].astype(BF16)
        at += blocks * dr
    if plan.rows > plan.used:
        chunk[:, plan.used :, :] = jnp.zeros((plan.reps, plan.rows - plan.used, LANES), BF16)
    core, me_y = me_g & 1, lax.shift_right_logical(me_g, 1)
    for h, out in ((0, keep_o), (1, send_o)):
        start = (core ^ h) * plan.half
        for z in range(plan.kz):
            for x in range(plan.kx):
                r = me_r ^ (z * 2 + x)
                for y in range(plan.ky):
                    q = me_y ^ y
                    m = plan.m1
                    at = ((x * plan.ky + y) * plan.kz + z) * m
                    row = pl.multiple_of(start + q * m, 16)
                    out[at : at + m, :] = chunk[r, pl.ds(row, m), :]
                    m = plan.m2
                    if m:
                        at = plan.p1 + ((y * plan.kx + x) * plan.kz + z) * m
                        row = pl.multiple_of(start + plan.ky * plan.m1 + q * m, 16)
                        out[at : at + m, :] = chunk[r, pl.ds(row, m), :]


def query_grad_body(peers, vec, grad, keep_o, send_o):
    turned = vec[...].T
    nq = keep_o.shape[2]
    for t in range(peers):
        part = (LOGIT_SCALE * mm(turned, grad[:, t * nq : (t + 1) * nq])).astype(BF16)
        (send_o if t & 1 else keep_o)[t // 2] = part


def query_core_body(keep, got, own_o, *sends):
    own_o[...] = keep[0].astype(F32) + got[0].astype(F32)
    for y, out in enumerate(sends):
        out[...] = (keep[y + 1].astype(F32) + got[y + 1].astype(F32)).astype(BF16)


def query_final_body(own, *rest):
    got, out = rest[:-1], rest[-1]
    total = own[...]
    for part in got:
        total += part[...].astype(F32)
    out[...] = total.T


def cut_body(cuts, *refs):
    n_in = len(refs) - len(cuts)
    for out, pieces in zip(refs[n_in:], cuts):
        for at, rows, terms in pieces:
            total = None
            for i, first in terms:
                part = refs[i][first : first + rows, :].astype(F32)
                total = part if total is None else total + part
            out[at : at + rows, :] = total.astype(out.dtype)


def cut(inputs, cuts):
    shapes = [sds((sum(p[1] for p in pieces), LANES), BF16) for pieces in cuts]
    return call(functools.partial(cut_body, cuts), shapes, inputs, vmem=8)


def final_body(plan, w_hot, w_mid, w_cold, cold_rows, *refs):
    pieces = refs[: plan.groups]
    o_in, o_out, o_hot, o_mid, o_cold, chunk = refs[plan.groups :]
    me_g = lax.axis_index("group")
    for t in range(plan.groups):
        h = (me_g & 1) ^ (t & 1)
        q = lax.shift_right_logical(me_g, 1) ^ (t >> 1)
        start = h * plan.half
        row = pl.multiple_of(start + q * plan.m1, 16)
        chunk[pl.ds(row, plan.m1), :] = pieces[t][0 : plan.m1, :].astype(F32)
        if plan.m2:
            row = pl.multiple_of(start + plan.ky * plan.m1 + q * plan.m2, 16)
            chunk[pl.ds(row, plan.m2), :] = pieces[t][plan.m1 :, :].astype(F32)
    hr, dr = plan.hr, plan.dr
    for b in range(plan.b_in):
        o_in[b * LANES : (b + 1) * LANES, :] = chunk[b * hr : (b + 1) * hr, :].T
    at = hr * plan.b_in
    for out, w in ((o_out, plan.b_out * LANES), (o_hot, w_hot), (o_mid, w_mid)):
        for b in range(w // LANES):
            out[:, b * LANES : (b + 1) * LANES] = chunk[at : at + dr, :]
            at += dr
    total = jnp.zeros((cold_rows, dr), F32)
    for _ in range(w_cold // LANES):
        turned = chunk[at : at + dr, :].T
        for k in range(LANES // cold_rows):
            total += turned[k * cold_rows : (k + 1) * cold_rows, :]
        at += dr
    o_cold[...] = total


def scatter_body(cold_width, rows_each, served, back, p_hot, *refs):
    outs, (pad, *wides), stages, sems = refs[:3], refs[3:7], refs[7:10], refs[10]
    width = p_hot.shape[1]
    slots = back.shape[0]
    w_mid, w_cold = outs[1].shape[1], outs[2].shape[1]
    cols = columns_of(served, pad)
    copies = []

    def widen(wide, row, part, values):
        w = values.shape[1]
        which = split_row(row, part)[0]
        for k in range(wide.shape[1] // w):
            wide[:, k * w : (k + 1) * w] = jnp.where(which == k, values, 0.0).astype(BF16)

    def put(out, stage, row, wide):
        w = out.shape[1]
        parts = wide.shape[1] // w
        part = out.shape[0] // parts
        low = split_row(row, part)[1]
        for at in range(0, part, rows_each):
            hit = ones_where(iota((rows_each, slots), 0) + at == low).astype(BF16)
            found = mm(hit, wide[...])
            for k in range(parts):
                rows = pl.ds(k * part + at, rows_each)
                stage[rows, :] = found[:, k * w : (k + 1) * w]
                copy = pltpu.make_async_copy(
                    stage.at[rows, :], out.at[rows, :], sems.at[len(copies)]
                )
                copy.start()
                copies.append(copy)

    wides[0][...] = mm(back[:, 0:width], p_hot[...], NT).astype(BF16)
    put(outs[0], stages[0], served[0], wides[0])
    mids = back[:, width : width + w_mid].astype(F32)
    widen(wides[1], cols[:, 1:2], outs[1].shape[0] * w_mid // wides[1].shape[1], mids)
    put(outs[1], stages[1], served[1], wides[1])
    lines = back[:, width + w_mid :].astype(F32)
    mine = lax.div(iota(lines.shape, 1), cold_width) == (cols[:, 2:3] & 3)
    row = lax.shift_right_logical(cols[:, 2:3], 2)
    part = outs[2].shape[0] * w_cold // wides[2].shape[1]
    widen(wides[2], row, part, jnp.where(mine, lines, 0.0))
    put(outs[2], stages[2], lax.shift_right_logical(served[2], 2), wides[2])
    for copy in copies:
        copy.wait()


def scatter_rows(served, back, proj_hot, shapes, cold_width):
    slots = served.shape[2]
    lanes = max(shape[1] for shape in shapes)
    parts = [parts_of(shape, lanes) for shape in shapes]
    rows_each = 256
    count = sum(shape[0] for shape in shapes) // rows_each
    vmem, hbm = pl.BlockSpec(memory_space=pltpu.VMEM), pl.BlockSpec(memory_space=pltpu.HBM)
    return pl.pallas_call(
        functools.partial(scatter_body, cold_width, rows_each),
        out_shape=[sds(shape, F32) for shape in shapes],
        in_specs=[vmem] * 3,
        out_specs=[hbm] * 3,
        scratch_shapes=[pltpu.VMEM((8, slots), jnp.int32)]
        + [pltpu.VMEM((slots, p * shape[1]), BF16) for p, shape in zip(parts, shapes)]
        + [pltpu.VMEM(shape, F32) for shape in shapes]
        + [pltpu.SemaphoreType.DMA((count,))],
        compiler_params=pltpu.CompilerParams(vmem_limit_bytes=24 * MIB),
        name="scatter_rows",
    )(served, back, proj_hot)


def local(
    groups,
    reps,
    table_hot,
    table_mid,
    table_cold,
    proj_hot,
    proj_mid,
    proj_cold,
    tower_in,
    tower_out,
    queries,
    labels,
    item_slot,
    item_block,
    serve_rows,
):
    devices = groups * reps
    slots = serve_rows.shape[2]
    cold_width, width = proj_cold.shape
    inner = tower_in.shape[1]
    items = item_slot.shape[2]
    nq = queries.shape[0]
    w_hot, w_mid, w_cold = table_hot.shape[1], table_mid.shape[1], table_cold.shape[1]
    raw_width = w_hot + w_mid + w_cold
    plan = Plan(groups, reps, width, inner, raw_width)

    def across_group(value, t):
        pairs = [(g * reps + r, (g ^ t) * reps + r) for g in range(groups) for r in range(reps)]
        return lax.ppermute(value, AXES, pairs)

    def across_rep(value, t):
        pairs = [(g * reps + r, g * reps + (r ^ t)) for g in range(groups) for r in range(reps)]
        return lax.ppermute(value, AXES, pairs)

    def to_all(rows):
        each = rows.reshape(devices, slots // devices, rows.shape[1])
        return lax.all_to_all(each, AXES, 0, 0, tiled=True).reshape(rows.shape)

    def to_group(value):
        found = {0: value}
        for t in range(2, groups, 2):
            found[t] = across_group(value, t)
        for t in range(0, groups, 2):
            found[t + 1] = across_group(found[t], 1)
        return [found[t] for t in range(groups)]

    served = jnp.transpose(serve_rows, (1, 0, 2))
    q_all = to_group(queries)
    rows = gather_rows(served, table_hot, table_mid, table_cold, cold_width)
    raw = to_all(rows)
    l_all = to_group(labels.reshape(1, nq))
    by_item, by_slot = call(
        functools.partial(count_body, slots),
        [sds((items, 3 * slots), BF16), sds((3 * slots, items), BF16)],
        [item_slot, item_block],
        scratch=[pltpu.VMEM((8, items), jnp.int32)],
        vmem=60,
    )
    blocks = groups * nq // QB
    pooled, resid, vec, stats, tops, grown = call(
        functools.partial(forward_body, groups),
        [
            sds((items, width), BF16),
            sds((items, width), F32),
            sds((items, width), BF16),
            sds((blocks, 3 * QB), F32),
            sds((blocks, items // IB * QB), F32),
            sds((items, groups * nq), F32),
        ],
        [raw, by_item, proj_hot, proj_mid, proj_cold, tower_in, tower_out] + q_all + l_all,
        scratch=[pltpu.VMEM((3 * slots, width), BF16)],
        vmem=8 * groups - 8,
    )
    s_all = [stats]
    for t in range(1, groups):
        s_all.append(across_group(stats, t))
    hidden, slope = call(
        slope_body,
        [sds((items, inner), BF16), sds((items, inner), F32)],
        [pooled, tower_in],
        vmem=12,
    )
    cut_rows = plan.p1 + plan.p2
    loss, grad, keep, send, back = call(
        functools.partial(backward_body, plan, groups),
        [
            sds((1, nq), F32),
            sds((items, groups * nq), BF16),
            sds((cut_rows, LANES), BF16),
            sds((cut_rows, LANES), BF16),
            sds((slots, width + w_mid + w_cold), BF16),
        ],
        s_all
        + q_all
        + l_all
        + [tops, grown, hidden, slope, resid, pooled, by_slot, raw]
        + [proj_hot, proj_mid, proj_cold, tower_in, tower_out],
        scratch=[
            pltpu.VMEM((items, width), BF16),
            pltpu.VMEM((items, inner), BF16),
            pltpu.VMEM((items, width), BF16),
            pltpu.VMEM((3 * slots, width), BF16),
            pltpu.VMEM((reps, plan.rows, LANES), BF16),
        ],
        vmem=8 * groups - 8,
    )
    back = to_all(back)

    got = across_group(send, 1)
    ky, kx, kz, m1, m2 = plan.ky, plan.kx, plan.kz, plan.m1, plan.m2

    n1, n2 = plan.p1 // kx, plan.p2 // ky
    cuts = []
    for x in range(kx):
        cuts.append([(0, n1, [(0, x * n1), (1, x * n1)])])
    for y in range(ky):
        cuts.append([(0, n2, [(0, plan.p1 + y * n2), (1, plan.p1 + y * n2)])])
    parts = cut([keep, got], cuts)
    a_keep, a_send = parts[0], parts[1:kx]
    b_keep, b_send = parts[kx], parts[kx + 1 :]
    a_got = [across_rep(v, x + 1) for x, v in enumerate(a_send)]
    b_got = [across_group(v, 2 * (y + 1)) for y, v in enumerate(b_send)]
    k1, k2 = n1 // ky, n2 // kx
    na, nb = 1 + len(a_got), 1 + len(b_got)
    cuts = [[(0, k1, [(i, y * k1) for i in range(na)])] for y in range(ky)]
    cuts += [[(0, k2, [(na + i, x * k2) for i in range(nb)])] for x in range(kx)]
    parts = cut([a_keep, *a_got, b_keep, *b_got], cuts)
    a_keep, a_send = parts[0], parts[1:ky]
    b_keep, b_send = parts[ky], parts[ky + 1 :]
    a_got = [across_group(v, 2 * (y + 1)) for y, v in enumerate(a_send)]
    b_got = [across_rep(v, x + 1) for x, v in enumerate(b_send)]
    na, nb = 1 + len(a_got), 1 + len(b_got)
    cuts = [
        [
            (0, m1, [(i, z * m1) for i in range(na)]),
            (m1, m2, [(na + i, z * m2) for i in range(nb)]),
        ]
        for z in range(kz)
    ]
    parts = cut([a_keep, *a_got, b_keep, *b_got], cuts)
    z_got = []
    for z in range(1, kz):
        z_got.append(across_rep(parts[z], 2 * z))
    mine = cut([parts[0], *z_got], [[(0, m1 + m2, [(i, 0) for i in range(kz)])]])[0]
    pieces = [mine] + [across_group(mine, t) for t in range(1, groups)]
    g_in, g_out, g_hot, g_mid, g_cold = call(
        functools.partial(final_body, plan, w_hot, w_mid, w_cold, cold_width),
        [
            sds((width, inner // reps), F32),
            sds((width // reps, inner), F32),
            sds((width // reps, w_hot), F32),
            sds((width // reps, w_mid), F32),
            sds((cold_width, width // reps), F32),
        ],
        pieces,
        scratch=[pltpu.VMEM((plan.rows, LANES), F32)],
        vmem=16,
    )

    q_keep, q_send = call(
        functools.partial(query_grad_body, groups),
        [sds((groups // 2, width, nq), BF16), sds((groups // 2, width, nq), BF16)],
        [vec, grad],
        vmem=16,
    )
    q_got = across_group(q_send, 1)
    own, *q_sends = call(
        query_core_body,
        [sds((width, nq), F32)] + [sds((width, nq), BF16)] * (ky - 1),
        [q_keep, q_got],
        vmem=16,
    )
    q_parts = [across_group(v, 2 * (y + 1)) for y, v in enumerate(q_sends)]
    query_grad = call(query_final_body, sds((nq, width), F32), [own, *q_parts], vmem=8)
    shapes = [table_hot.shape, table_mid.shape, table_cold.shape]
    o_hot, o_mid, o_cold = scatter_rows(served, back, proj_hot, shapes, cold_width)
    return (
        loss.reshape(nq),
        query_grad,
        o_hot,
        o_mid,
        o_cold,
        g_hot.T,
        g_mid.T,
        g_cold,
        g_in,
        g_out.T,
    )


def solution(mesh):
    split = P(AXES, None)
    deep = P(AXES, None, None)

    def body(*args):
        return local(mesh.shape["group"], mesh.shape["rep"], *args)

    return jax.shard_map(
        body,
        mesh=mesh,
        in_specs=(split, split, split, P(), P(), P(), P(), P(), split, P(AXES), deep, deep, deep),
        out_specs=(P(AXES), split, split, split, split) + (P(None, "rep"),) * 5,
        check_vma=False,
    )
```

```python
import functools

import jax
import jax.numpy as jnp
from jax import lax
from jax.experimental import pallas as pl
from jax.experimental.pallas import tpu as pltpu
from jax.sharding import PartitionSpec as P


NORM_EPS = 1e-06
LOGIT_SCALE = 0.2
LOG2_E = 1.4426950408889634
AXES = ("group", "rep")
LANES = 128
QB = 256
IB = 256
MIB = 1 << 20
F32 = jnp.float32
BF16 = jnp.bfloat16

NN = (((1,), (0,)), ((), ()))
NT = (((1,), (1,)), ((), ()))
TN = (((0,), (0,)), ((), ()))


def mm(left, right, dims=NN):
    return lax.dot_general(left, right, dims, preferred_element_type=F32)


def ones_where(mask):
    return jnp.where(mask, jnp.float32(1), jnp.float32(0))


def iota(shape, dim):
    return lax.broadcasted_iota(jnp.int32, shape, dim)


def call(body, out_shape, inputs, far=(), scratch=(), vmem=40):
    spec = pl.BlockSpec(memory_space=pltpu.VMEM)
    return pl.pallas_call(
        body,
        out_shape=out_shape,
        in_specs=[spec] * len(inputs) + [pl.BlockSpec(memory_space=pltpu.HBM)] * len(far),
        out_specs=jax.tree.map(lambda _: spec, out_shape),
        scratch_shapes=list(scratch),
        compiler_params=pltpu.CompilerParams(vmem_limit_bytes=vmem * MIB),
    )(*inputs, *far)


def sds(shape, dtype):
    return jax.ShapeDtypeStruct(shape, dtype)


def columns_of(served, pad_ref):
    pad_ref[...] = jnp.zeros_like(pad_ref)
    for k in range(served.shape[0]):
        pad_ref[k : k + 1, :] = served[k]
    return pad_ref[...].T


def parts_of(shape, lanes):
    return max(1, lanes // shape[1])


def split_row(row, part):
    return lax.div(row, part), lax.rem(row, part)


def gather_body(cold_width, parts, served, hot, mid, cold, out, pad, asked, v_hot, v_mid, v_cold, sems):
    copies = [
        pltpu.make_async_copy(source, target, sems.at[k])
        for k, (source, target) in enumerate(
            ((served, asked), (hot, v_hot), (mid, v_mid), (cold, v_cold))
        )
    ]
    for copy in copies:
        copy.start()
    copies[0].wait()
    idx = columns_of(asked, pad)
    slots = out.shape[0]

    def pick(k, table, row, w):
        part = table.shape[0] // parts[k]
        which, low = split_row(row, part)
        hit = ones_where(iota((slots, part), 1) == low).astype(BF16)
        copies[k + 1].wait()
        wide = [table[p * part : (p + 1) * part, :] for p in range(parts[k])]
        found = mm(hit, wide[0] if parts[k] == 1 else jnp.concatenate(wide, axis=1))
        value = found[:, 0:w]
        for p in range(1, parts[k]):
            value = jnp.where(which == p, found[:, p * w : (p + 1) * w], value)
        return value

    w_hot, w_mid, w_cold = hot.shape[1], mid.shape[1], cold.shape[1]
    out[:, 0:w_hot] = pick(0, v_hot, idx[:, 0:1], w_hot).astype(BF16)
    out[:, w_hot : w_hot + w_mid] = pick(1, v_mid, idx[:, 1:2], w_mid).astype(BF16)
    row = idx[:, 2:3]
    lines = pick(2, v_cold, lax.shift_right_logical(row, 2), w_cold)
    mine = lax.div(iota(lines.shape, 1), cold_width) == (row & 3)
    out[:, w_hot + w_mid :] = jnp.where(mine, lines, 0.0).astype(BF16)


def gather_rows(served, table_hot, table_mid, table_cold, cold_width):
    slots = served.shape[2]
    tables = (table_hot, table_mid, table_cold)
    width = sum(table.shape[1] for table in tables)
    lanes = max(table.shape[1] for table in tables)
    parts = [parts_of(table.shape, lanes) for table in tables]
    hbm = pl.BlockSpec(memory_space=pltpu.HBM)
    vmem = pl.BlockSpec(memory_space=pltpu.VMEM)
    return pl.pallas_call(
        functools.partial(gather_body, cold_width, parts),
        out_shape=sds((slots, width), BF16),
        in_specs=[hbm, hbm, hbm, hbm],
        out_specs=vmem,
        scratch_shapes=[pltpu.VMEM((8, slots), jnp.int32), pltpu.VMEM(served.shape, jnp.int32)]
        + [pltpu.VMEM(table.shape, BF16) for table in tables]
        + [pltpu.SemaphoreType.DMA((4,))],
        compiler_params=pltpu.CompilerParams(vmem_limit_bytes=60 * MIB),
        name="gather_rows",
    )(served, *tables)


def slot_of(slots, item_slot, item_block):
    return item_block[0] * slots + item_slot[0]


def count_body(slots, item_slot, item_block, by_item, by_slot, pad):
    fields, items = item_slot.shape[1], item_slot.shape[2]
    which = slot_of(slots, item_slot, item_block)
    count_slots(which, by_slot)
    pad[...] = jnp.zeros_like(pad)
    pad[0:fields, :] = which
    cols = pad[...].T
    for base in range(0, by_item.shape[1], QB):
        lanes = iota((items, QB), 1) + base
        total = jnp.zeros((items, QB), F32)
        for f in range(fields):
            total += ones_where(lanes == cols[:, f : f + 1])
        by_item[:, base : base + QB] = total.astype(BF16)


def count_slots(which, by_slot):
    for base in range(0, by_slot.shape[0], QB):
        rows = iota((QB, which.shape[1]), 0) + base
        total = jnp.zeros((QB, which.shape[1]), F32)
        for f in range(which.shape[0]):
            total += ones_where(rows == which[f : f + 1, :])
        by_slot[base : base + QB, :] = total.astype(BF16)


def tall(weight, times):
    return jnp.concatenate([weight] * times, axis=0)


def label_rows(label, base, jj):
    row = label[0:1, jj * QB : (jj + 1) * QB] - base
    return row - iota((8, QB), 0)


def hits(rows, label, at):
    first = 8 * iota((rows // 8, 8, QB), 0) + at
    return first == label[None]


def by_eight(value):
    return value.reshape(value.shape[0] // 8, 8, value.shape[1])


def sigmoid(value):
    return 0.5 + 0.5 * jnp.tanh(0.5 * value)


def forward_body(peers, raw, counts, p_hot, p_mid, p_cold, t_in, t_out, *rest):
    queries, labels = rest[:peers], rest[peers : 2 * peers]
    pooled_o, resid_o, vec_o, stats_o, tops_o, exp_o, table = rest[2 * peers :]
    slots = raw.shape[0]
    w_hot, w_mid = p_hot.shape[0], p_mid.shape[0]
    w_cold = raw.shape[1] - w_hot - w_mid
    table[0:slots, :] = mm(raw[:, 0:w_hot], p_hot[...]).astype(BF16)
    table[slots : 2 * slots, :] = mm(raw[:, w_hot : w_hot + w_mid], p_mid[...]).astype(BF16)
    table[2 * slots :, :] = mm(
        raw[:, w_hot + w_mid :], tall(p_cold[...], w_cold // p_cold.shape[0])
    ).astype(BF16)
    items = counts.shape[0]
    base = lax.axis_index("group") * items
    nq = queries[0].shape[0]
    per = nq // QB
    blocks = [(t, jj) for t in range(peers) for jj in range(per)]
    wanted = [label_rows(labels[t], base, jj) for t, jj in blocks]
    kept = [[] for _ in blocks]
    step = t_in.shape[1] // 4

    def tower(ib):
        rows = slice(ib * IB, (ib + 1) * IB)
        pooled = mm(counts[rows, :], table[...]).astype(BF16)
        pooled_o[rows, :] = pooled
        resid = pooled.astype(F32)
        yield
        for at in range(0, t_in.shape[1], step):
            pre = mm(pooled, t_in[:, at : at + step])
            hidden = (pre * sigmoid(pre)).astype(BF16)
            yield
            resid += mm(hidden, t_out[at : at + step, :])
        inv = lax.rsqrt(jnp.mean(resid * resid, axis=1, keepdims=True) + NORM_EPS)
        resid_o[rows, :] = resid
        vec_o[rows, :] = (resid * inv).astype(BF16)

    def score(ib, j):
        at = ib * IB
        rows = slice(at, at + IB)
        t, jj = blocks[j]
        s = mm(vec_o[rows, :], queries[t][jj * QB : (jj + 1) * QB, :], NT)
        top = jnp.max(s, axis=0, keepdims=True)
        grown = jnp.exp2((s - top) * (LOGIT_SCALE * LOG2_E))
        total = jnp.sum(grown, axis=0, keepdims=True)
        picked = jnp.where(hits(IB, wanted[j], at), by_eight(s), 0.0)
        picked = jnp.sum(jnp.sum(picked, axis=0), axis=0, keepdims=True)
        exp_o[rows, j * QB : (j + 1) * QB] = grown
        top = LOGIT_SCALE * top
        tops_o[j : j + 1, ib * QB : (ib + 1) * QB] = top
        kept[j].append((top, total, LOGIT_SCALE * picked))

    for _ in tower(0):
        pass
    for ib in range(items // IB):
        ahead = tower(ib + 1) if ib + 1 < items // IB else iter(())
        for j in range(len(blocks)):
            next(ahead, None)
            score(ib, j)
        for _ in ahead:
            pass
    for j, parts in enumerate(kept):
        top = functools.reduce(jnp.maximum, [part[0] for part in parts])
        stats_o[j : j + 1, 0:QB] = top
        stats_o[j : j + 1, QB : 2 * QB] = sum(p[1] * jnp.exp(p[0] - top) for p in parts)
        stats_o[j : j + 1, 2 * QB :] = sum(part[2] for part in parts)


def slope_body(pooled, t_in, hidden_o, slope_o, turned_o):
    turned_o[...] = pooled[...].T
    for at in range(0, pooled.shape[0], IB):
        rows = slice(at, at + IB)
        pre = mm(pooled[rows, :], t_in[...])
        sig = sigmoid(pre)
        hidden_o[rows, :] = (pre * sig).astype(BF16)
        slope_o[rows, :] = sig * (1.0 + pre * (1.0 - sig))


class Plan:
    def __init__(self, groups, reps, width, inner, raw_width):
        self.groups, self.reps = groups, reps
        self.ky = groups // 2
        self.kx, self.kz = 2, reps // 2
        self.hr = inner // reps
        self.dr = width // reps
        self.b_in = width // LANES
        self.b_out = inner // LANES
        self.b_raw = raw_width // LANES
        rows = self.hr * self.b_in + self.dr * (self.b_out + self.b_raw)
        unit = 16 * self.ky
        units = -(-rows // (2 * unit))
        self.half = units * unit
        self.m1 = -(-units // 2) * 16
        self.m2 = units * 16 - self.m1
        self.rows = 2 * self.half
        self.used = rows
        self.p1 = reps * self.ky * self.m1
        self.p2 = reps * self.ky * self.m2


def backward_body(plan, peers, *refs):
    stats, refs = refs[:peers], refs[peers:]
    queries, refs = refs[:peers], refs[peers:]
    labels, refs = refs[:peers], refs[peers:]
    tops_r, grown, hidden, slope, resid, turned, by_slot, raw = refs[:8]
    p_hot, p_mid, p_cold, t_in, t_out = refs[8:13]
    loss_o, grad_o, keep_o, send_o, back_o = refs[13:18]
    low_s, pre_s, pgrad_s, slot_s, chunk = refs[18:]
    width, items = turned.shape
    nq = queries[0].shape[0]
    per = nq // QB
    me_g, me_r = lax.axis_index("group"), lax.axis_index("rep")
    base = me_g * items
    log_totals, wanted = [], []
    for t in range(peers):
        for jj in range(per):
            rows = [(t ^ s) * per + jj for s in range(peers)]
            tops = [stats[s][rows[s] : rows[s] + 1, 0:QB] for s in range(peers)]
            totals = [stats[s][rows[s] : rows[s] + 1, QB : 2 * QB] for s in range(peers)]
            top = functools.reduce(jnp.maximum, tops)
            total = sum(tot * jnp.exp(m - top) for m, tot in zip(tops, totals))
            log_total = top + jnp.log(total)
            if t == 0:
                picked = sum(stats[s][rows[s] : rows[s] + 1, 2 * QB :] for s in range(peers))
                loss_o[0:1, jj * QB : (jj + 1) * QB] = log_total - picked
            log_totals.append(log_total)
            wanted.append(label_rows(labels[t], base, jj))
    for at in range(0, items, IB):
        rows = slice(at, at + IB)
        for j, log_total in enumerate(log_totals):
            ib = at // IB
            scale = jnp.exp(tops_r[j : j + 1, ib * QB : (ib + 1) * QB] - log_total)
            share = by_eight(grown[rows, j * QB : (j + 1) * QB] * scale)
            share = share - ones_where(hits(IB, wanted[j], at))
            grad_o[rows, j * QB : (j + 1) * QB] = share.reshape(IB, QB).astype(BF16)
        vgrad = mm(grad_o[rows, 0:nq], queries[0][...])
        for t in range(1, peers):
            vgrad += mm(grad_o[rows, t * nq : (t + 1) * nq], queries[t][...])
        vgrad = LOGIT_SCALE * vgrad
        res = resid[rows, :]
        inv = lax.rsqrt(jnp.mean(res * res, axis=1, keepdims=True) + NORM_EPS)
        dot_wide = jnp.sum(vgrad * res, axis=1, keepdims=True)
        wide = inv * vgrad - (inv * inv * inv / width * dot_wide) * res
        low = wide.astype(BF16)
        low_s[rows, :] = low
        pre_g = (mm(low, t_out[...], NT) * slope[rows, :]).astype(BF16)
        pre_s[rows, :] = pre_g
        pgrad_s[rows, :] = (mm(pre_g, t_in[...], NT) + wide).astype(BF16)
    slots = raw.shape[0]
    w_hot, w_mid = p_hot.shape[0], p_mid.shape[0]
    w_cold = raw.shape[1] - w_hot - w_mid
    slot_s[...] = mm(by_slot[...], pgrad_s[...]).astype(BF16)
    back_o[:, 0:width] = slot_s[0:slots, :]
    back_o[:, width : width + w_mid] = mm(slot_s[slots : 2 * slots, :], p_mid[...], NT).astype(BF16)
    back_o[:, width + w_mid :] = mm(
        slot_s[2 * slots :, :], tall(p_cold[...], w_cold // p_cold.shape[0]), NT
    ).astype(BF16)

    g_in = mm(turned[...], pre_s[...]).T
    hr, dr = plan.hr, plan.dr
    for r in range(plan.reps):
        for b in range(plan.b_in):
            chunk[r, b * hr : (b + 1) * hr, :] = g_in[
                r * hr : (r + 1) * hr, b * LANES : (b + 1) * LANES
            ].astype(BF16)
    at = hr * plan.b_in
    g_out = mm(low_s[...], hidden[...], TN)
    parts = [(g_out, plan.b_out)]
    lane = 0
    for b, w in enumerate((w_hot, w_mid, w_cold)):
        parts.append(
            (mm(slot_s[b * slots : (b + 1) * slots, :], raw[:, lane : lane + w], TN), w // LANES)
        )
        lane += w
    for value, blocks in parts:
        for r in range(plan.reps):
            for b in range(blocks):
                chunk[r, at + b * dr : at + (b + 1) * dr, :] = value[
                    r * dr : (r + 1) * dr, b * LANES : (b + 1) * LANES
                ].astype(BF16)
        at += blocks * dr
    if plan.rows > plan.used:
        chunk[:, plan.used :, :] = jnp.zeros((plan.reps, plan.rows - plan.used, LANES), BF16)
    core, me_y = me_g & 1, lax.shift_right_logical(me_g, 1)
    for h, out in ((0, keep_o), (1, send_o)):
        start = (core ^ h) * plan.half
        for z in range(plan.kz):
            for x in range(plan.kx):
                r = me_r ^ (z * 2 + x)
                for y in range(plan.ky):
                    q = me_y ^ y
                    m = plan.m1
                    at = ((x * plan.ky + y) * plan.kz + z) * m
                    row = pl.multiple_of(start + q * m, 16)
                    out[at : at + m, :] = chunk[r, pl.ds(row, m), :]
                    m = plan.m2
                    if m:
                        at = plan.p1 + ((y * plan.kx + x) * plan.kz + z) * m
                        row = pl.multiple_of(start + plan.ky * plan.m1 + q * m, 16)
                        out[at : at + m, :] = chunk[r, pl.ds(row, m), :]


def query_grad_body(peers, vec, grad, keep_o, send_o):
    turned = vec[...].T
    nq = keep_o.shape[2]
    for t in range(peers):
        part = (LOGIT_SCALE * mm(turned, grad[:, t * nq : (t + 1) * nq])).astype(BF16)
        (send_o if t & 1 else keep_o)[t // 2] = part


def query_core_body(keep, got, own_o, *sends):
    own_o[...] = keep[0].astype(F32) + got[0].astype(F32)
    for y, out in enumerate(sends):
        out[...] = (keep[y + 1].astype(F32) + got[y + 1].astype(F32)).astype(BF16)


def query_final_body(own, *rest):
    got, out = rest[:-1], rest[-1]
    total = own[...]
    for part in got:
        total += part[...].astype(F32)
    out[...] = total.T


def cut_body(cuts, *refs):
    n_in = len(refs) - len(cuts)
    for out, pieces in zip(refs[n_in:], cuts):
        for at, rows, terms in pieces:
            total = None
            for i, first in terms:
                part = refs[i][first : first + rows, :].astype(F32)
                total = part if total is None else total + part
            out[at : at + rows, :] = total.astype(out.dtype)


def cut(inputs, cuts):
    shapes = [sds((sum(p[1] for p in pieces), LANES), BF16) for pieces in cuts]
    return call(functools.partial(cut_body, cuts), shapes, inputs, vmem=8)


def final_body(plan, w_hot, w_mid, w_cold, cold_rows, *refs):
    pieces = refs[: plan.groups]
    o_in, o_out, o_hot, o_mid, o_cold, chunk = refs[plan.groups :]
    me_g = lax.axis_index("group")
    for t in range(plan.groups):
        h = (me_g & 1) ^ (t & 1)
        q = lax.shift_right_logical(me_g, 1) ^ (t >> 1)
        start = h * plan.half
        row = pl.multiple_of(start + q * plan.m1, 16)
        chunk[pl.ds(row, plan.m1), :] = pieces[t][0 : plan.m1, :].astype(F32)
        if plan.m2:
            row = pl.multiple_of(start + plan.ky * plan.m1 + q * plan.m2, 16)
            chunk[pl.ds(row, plan.m2), :] = pieces[t][plan.m1 :, :].astype(F32)
    hr, dr = plan.hr, plan.dr
    for b in range(plan.b_in):
        o_in[b * LANES : (b + 1) * LANES, :] = chunk[b * hr : (b + 1) * hr, :].T
    at = hr * plan.b_in
    for out, w in ((o_out, plan.b_out * LANES), (o_hot, w_hot), (o_mid, w_mid)):
        for b in range(w // LANES):
            out[:, b * LANES : (b + 1) * LANES] = chunk[at : at + dr, :]
            at += dr
    total = jnp.zeros((cold_rows, dr), F32)
    for _ in range(w_cold // LANES):
        turned = chunk[at : at + dr, :].T
        for k in range(LANES // cold_rows):
            total += turned[k * cold_rows : (k + 1) * cold_rows, :]
        at += dr
    o_cold[...] = total


def scatter_body(cold_width, rows_each, served, back, p_hot, *refs):
    outs, (pad, *wides), stages, sems = refs[:3], refs[3:7], refs[7:10], refs[10]
    width = p_hot.shape[1]
    slots = back.shape[0]
    w_mid, w_cold = outs[1].shape[1], outs[2].shape[1]
    cols = columns_of(served, pad)
    copies = []

    def widen(wide, row, part, values):
        w = values.shape[1]
        which = split_row(row, part)[0]
        for k in range(wide.shape[1] // w):
            wide[:, k * w : (k + 1) * w] = jnp.where(which == k, values, 0.0).astype(BF16)

    def put(out, stage, row, wide):
        w = out.shape[1]
        parts = wide.shape[1] // w
        part = out.shape[0] // parts
        low = split_row(row, part)[1]
        for at in range(0, part, rows_each):
            hit = ones_where(iota((rows_each, slots), 0) + at == low).astype(BF16)
            found = mm(hit, wide[...])
            for k in range(parts):
                rows = pl.ds(k * part + at, rows_each)
                stage[rows, :] = found[:, k * w : (k + 1) * w]
                copy = pltpu.make_async_copy(
                    stage.at[rows, :], out.at[rows, :], sems.at[len(copies)]
                )
                copy.start()
                copies.append(copy)

    wides[0][...] = mm(back[:, 0:width], p_hot[...], NT).astype(BF16)
    put(outs[0], stages[0], served[0], wides[0])
    mids = back[:, width : width + w_mid].astype(F32)
    widen(wides[1], cols[:, 1:2], outs[1].shape[0] * w_mid // wides[1].shape[1], mids)
    put(outs[1], stages[1], served[1], wides[1])
    lines = back[:, width + w_mid :].astype(F32)
    mine = lax.div(iota(lines.shape, 1), cold_width) == (cols[:, 2:3] & 3)
    row = lax.shift_right_logical(cols[:, 2:3], 2)
    part = outs[2].shape[0] * w_cold // wides[2].shape[1]
    widen(wides[2], row, part, jnp.where(mine, lines, 0.0))
    put(outs[2], stages[2], lax.shift_right_logical(served[2], 2), wides[2])
    for copy in copies:
        copy.wait()


def scatter_rows(served, back, proj_hot, shapes, cold_width):
    slots = served.shape[2]
    lanes = max(shape[1] for shape in shapes)
    parts = [parts_of(shape, lanes) for shape in shapes]
    rows_each = 256
    count = sum(shape[0] for shape in shapes) // rows_each
    vmem, hbm = pl.BlockSpec(memory_space=pltpu.VMEM), pl.BlockSpec(memory_space=pltpu.HBM)
    return pl.pallas_call(
        functools.partial(scatter_body, cold_width, rows_each),
        out_shape=[sds(shape, F32) for shape in shapes],
        in_specs=[vmem] * 3,
        out_specs=[hbm] * 3,
        scratch_shapes=[pltpu.VMEM((8, slots), jnp.int32)]
        + [pltpu.VMEM((slots, p * shape[1]), BF16) for p, shape in zip(parts, shapes)]
        + [pltpu.VMEM(shape, F32) for shape in shapes]
        + [pltpu.SemaphoreType.DMA((count,))],
        compiler_params=pltpu.CompilerParams(vmem_limit_bytes=24 * MIB),
        name="scatter_rows",
    )(served, back, proj_hot)


def local(
    groups,
    reps,
    table_hot,
    table_mid,
    table_cold,
    proj_hot,
    proj_mid,
    proj_cold,
    tower_in,
    tower_out,
    queries,
    labels,
    item_slot,
    item_block,
    serve_rows,
):
    devices = groups * reps
    slots = serve_rows.shape[2]
    cold_width, width = proj_cold.shape
    inner = tower_in.shape[1]
    items = item_slot.shape[2]
    nq = queries.shape[0]
    w_hot, w_mid, w_cold = table_hot.shape[1], table_mid.shape[1], table_cold.shape[1]
    raw_width = w_hot + w_mid + w_cold
    plan = Plan(groups, reps, width, inner, raw_width)

    def across_group(value, t):
        pairs = [(g * reps + r, (g ^ t) * reps + r) for g in range(groups) for r in range(reps)]
        return lax.ppermute(value, AXES, pairs)

    def across_rep(value, t):
        pairs = [(g * reps + r, g * reps + (r ^ t)) for g in range(groups) for r in range(reps)]
        return lax.ppermute(value, AXES, pairs)

    def to_all(rows):
        each = rows.reshape(devices, slots // devices, rows.shape[1])
        return lax.all_to_all(each, AXES, 0, 0, tiled=True).reshape(rows.shape)

    def to_group(value):
        found = {0: value}
        for t in range(2, groups, 2):
            found[t] = across_group(value, t)
        for t in range(0, groups, 2):
            found[t + 1] = across_group(found[t], 1)
        return [found[t] for t in range(groups)]

    served = jnp.transpose(serve_rows, (1, 0, 2))
    q_all = to_group(queries)
    rows = gather_rows(served, table_hot, table_mid, table_cold, cold_width)
    raw = to_all(rows)
    l_all = to_group(labels.reshape(1, nq))
    by_item, by_slot = call(
        functools.partial(count_body, slots),
        [sds((items, 3 * slots), BF16), sds((3 * slots, items), BF16)],
        [item_slot, item_block],
        scratch=[pltpu.VMEM((8, items), jnp.int32)],
        vmem=60,
    )
    blocks = groups * nq // QB
    pooled, resid, vec, stats, tops, grown = call(
        functools.partial(forward_body, groups),
        [
            sds((items, width), BF16),
            sds((items, width), F32),
            sds((items, width), BF16),
            sds((blocks, 3 * QB), F32),
            sds((blocks, items // IB * QB), F32),
            sds((items, groups * nq), F32),
        ],
        [raw, by_item, proj_hot, proj_mid, proj_cold, tower_in, tower_out] + q_all + l_all,
        scratch=[pltpu.VMEM((3 * slots, width), BF16)],
        vmem=8 * groups - 8,
    )
    s_all = [stats]
    for t in range(1, groups):
        s_all.append(across_group(stats, t))
    hidden, slope, turned = call(
        slope_body,
        [sds((items, inner), BF16), sds((items, inner), F32), sds((width, items), BF16)],
        [pooled, tower_in],
        vmem=12,
    )
    cut_rows = plan.p1 + plan.p2
    loss, grad, keep, send, back = call(
        functools.partial(backward_body, plan, groups),
        [
            sds((1, nq), F32),
            sds((items, groups * nq), BF16),
            sds((cut_rows, LANES), BF16),
            sds((cut_rows, LANES), BF16),
            sds((slots, width + w_mid + w_cold), BF16),
        ],
        s_all
        + q_all
        + l_all
        + [tops, grown, hidden, slope, resid, turned, by_slot, raw]
        + [proj_hot, proj_mid, proj_cold, tower_in, tower_out],
        scratch=[
            pltpu.VMEM((items, width), BF16),
            pltpu.VMEM((items, inner), BF16),
            pltpu.VMEM((items, width), BF16),
            pltpu.VMEM((3 * slots, width), BF16),
            pltpu.VMEM((reps, plan.rows, LANES), BF16),
        ],
        vmem=8 * groups - 8,
    )
    back = to_all(back)

    got = across_group(send, 1)
    ky, kx, kz, m1, m2 = plan.ky, plan.kx, plan.kz, plan.m1, plan.m2

    n1, n2 = plan.p1 // kx, plan.p2 // ky
    cuts = []
    for x in range(kx):
        cuts.append([(0, n1, [(0, x * n1), (1, x * n1)])])
    for y in range(ky):
        cuts.append([(0, n2, [(0, plan.p1 + y * n2), (1, plan.p1 + y * n2)])])
    parts = cut([keep, got], cuts)
    a_keep, a_send = parts[0], parts[1:kx]
    b_keep, b_send = parts[kx], parts[kx + 1 :]
    a_got = [across_rep(v, x + 1) for x, v in enumerate(a_send)]
    b_got = [across_group(v, 2 * (y + 1)) for y, v in enumerate(b_send)]
    k1, k2 = n1 // ky, n2 // kx
    na, nb = 1 + len(a_got), 1 + len(b_got)
    cuts = [[(0, k1, [(i, y * k1) for i in range(na)])] for y in range(ky)]
    cuts += [[(0, k2, [(na + i, x * k2) for i in range(nb)])] for x in range(kx)]
    parts = cut([a_keep, *a_got, b_keep, *b_got], cuts)
    a_keep, a_send = parts[0], parts[1:ky]
    b_keep, b_send = parts[ky], parts[ky + 1 :]
    a_got = [across_group(v, 2 * (y + 1)) for y, v in enumerate(a_send)]
    b_got = [across_rep(v, x + 1) for x, v in enumerate(b_send)]
    na, nb = 1 + len(a_got), 1 + len(b_got)
    cuts = [
        [
            (0, m1, [(i, z * m1) for i in range(na)]),
            (m1, m2, [(na + i, z * m2) for i in range(nb)]),
        ]
        for z in range(kz)
    ]
    parts = cut([a_keep, *a_got, b_keep, *b_got], cuts)
    z_got = []
    for z in range(1, kz):
        z_got.append(across_rep(parts[z], 2 * z))
    mine = cut([parts[0], *z_got], [[(0, m1 + m2, [(i, 0) for i in range(kz)])]])[0]
    pieces = [mine] + [across_group(mine, t) for t in range(1, groups)]
    g_in, g_out, g_hot, g_mid, g_cold = call(
        functools.partial(final_body, plan, w_hot, w_mid, w_cold, cold_width),
        [
            sds((width, inner // reps), F32),
            sds((width // reps, inner), F32),
            sds((width // reps, w_hot), F32),
            sds((width // reps, w_mid), F32),
            sds((cold_width, width // reps), F32),
        ],
        pieces,
        scratch=[pltpu.VMEM((plan.rows, LANES), F32)],
        vmem=16,
    )

    q_keep, q_send = call(
        functools.partial(query_grad_body, groups),
        [sds((groups // 2, width, nq), BF16), sds((groups // 2, width, nq), BF16)],
        [vec, grad],
        vmem=16,
    )
    q_got = across_group(q_send, 1)
    own, *q_sends = call(
        query_core_body,
        [sds((width, nq), F32)] + [sds((width, nq), BF16)] * (ky - 1),
        [q_keep, q_got],
        vmem=16,
    )
    q_parts = [across_group(v, 2 * (y + 1)) for y, v in enumerate(q_sends)]
    query_grad = call(query_final_body, sds((nq, width), F32), [own, *q_parts], vmem=8)
    shapes = [table_hot.shape, table_mid.shape, table_cold.shape]
    o_hot, o_mid, o_cold = scatter_rows(served, back, proj_hot, shapes, cold_width)
    return (
        loss.reshape(nq),
        query_grad,
        o_hot,
        o_mid,
        o_cold,
        g_hot.T,
        g_mid.T,
        g_cold,
        g_in,
        g_out.T,
    )


def solution(mesh):
    split = P(AXES, None)
    deep = P(AXES, None, None)

    def body(*args):
        return local(mesh.shape["group"], mesh.shape["rep"], *args)

    return jax.shard_map(
        body,
        mesh=mesh,
        in_specs=(split, split, split, P(), P(), P(), P(), P(), split, P(AXES), deep, deep, deep),
        out_specs=(P(AXES), split, split, split, split) + (P(None, "rep"),) * 5,
        check_vma=False,
    )
```
